512 devices in a mesh: chan: 2 (over y), row: 128 (over z, x), col: 2 (over core).
Axes of the slice: x: 8, y: 2, z: 16, core: 2. Of those that a mesh axis runs over, the one named last changes fastest.
The devices are a block of a 8x16x16 slice.
Arguments:
- hamiltonian_rows: float32 [256, 2, 2, 65536], P('chan', 'col', None, 'row'), parts along dimension 0, may hold values from -2 to 2, as said below
- current_block: float32 [131072, 256], P(('chan', 'row', 'col')), parts along dimension 0, may hold values from -6 to 6
- correction_block: float32 [131072, 256], P(('chan', 'row', 'col')), parts along dimension 0, may hold values from -6 to 6
- previous_block: float32 [131072, 256], P(('chan', 'row', 'col')), parts along dimension 0, may hold values from -6 to 6
- ritz_values: float32 [512], P('chan'), parts along dimension 0, may hold values from -2 to 2
- mixing_coeffs: float32 [1536, 256], P('chan'), parts along dimension 0, may hold values from -0.21875 to 0.21875
Outputs:
- next_block: float32 [1024, 256], P(('chan', 'row', 'col')), parts along dimension 0
- next_direction: float32 [1024, 256], P(('chan', 'row', 'col')), parts along dimension 0
- next_correction: float32 [1024, 256], P(('chan', 'row', 'col')), parts along dimension 0
- ritz_matrix: float32 [512, 256], P('chan'), parts along dimension 0
- metric_matrix: float32 [512, 256], P('chan'), parts along dimension 0
The draws below stay inside these ranges and needn't reach their ends.
There are 2 independent parts, one for each index of `chan`. The reference program is written for one: setup_inputs(seed, part) draws one part's arguments, and reference() takes and returns one part's arrays. A program takes and returns all parts, laid end to end along the dimension named above; each array names one. Nothing has to cross between parts.
Inputs may be any that keep to these rules, and one draw needn't show every extreme that they name: hamiltonian_rows[a, b, j, :] is row (a * 2 + b) * 256 + j of the channel's Hamiltonian; its entry in that row's own column is the onsite energy.
All inputs are finite; a program needn't handle non-finite values.
Results may differ from the reference program's by a relative error of at most 0.00008.
Values sent between devices are 32-bit elements; how exact they have to be, the bound alone decides.
A program may use at most 64 MiB of HBM per device.

```python
import math
import jax
import jax.numpy as jnp
from jax import lax

N = 65536
BLOCK = 256
OUT_DEV = 2
N_ROW = 128
N_COL = 2


def draw_hamiltonian_rows(key, part):
    first_key = jax.random.fold_in(key, 11)
    second_key = jax.random.fold_in(key, 12)
    shape = (N_ROW, N_COL, OUT_DEV, N)
    coupling = jax.random.truncated_normal(first_key, -6.0, 6.0, shape, jnp.float32) / math.sqrt(N)
    block_index = lax.broadcasted_iota(jnp.int32, shape, 0) * N_COL + lax.broadcasted_iota(jnp.int32, shape, 1)
    slot_index = lax.broadcasted_iota(jnp.int32, shape, 2)
    column_index = lax.broadcasted_iota(jnp.int32, shape, 3)
    position = (block_index * OUT_DEV + slot_index).astype(jnp.float32) / (N_ROW * N_COL * OUT_DEV)
    row_scale = jnp.exp(position * math.log(3.0))
    onsite = jax.random.uniform(second_key, (N_ROW, N_COL, OUT_DEV, 1), jnp.float32, -2.0, 2.0)
    own_column = column_index == block_index * (N // (N_ROW * N_COL)) + slot_index
    return jnp.where(own_column, onsite, coupling * row_scale)


def block_scale(rng, dims, cuts, smallest, largest):
    def one(dim, blocks):
        heights = jax.random.uniform(jax.random.fold_in(jax.random.fold_in(rng, 6), dim), (blocks,), jnp.float32, smallest / len(cuts), largest / len(cuts))
        return jnp.repeat(jnp.exp(heights), dims[dim] // blocks).reshape((-1,) + (1,) * (len(dims) - dim - 1))

    factor_of = one(*cuts[0])
    for cut in cuts[1:]:
        factor_of = factor_of * one(*cut)
    return factor_of


def normal_values(rng, shape, deviation, limit, cuts=(), held_as=jnp.bfloat16):
    entries = deviation * jax.random.normal(rng, shape, jnp.float32)
    if cuts:
        entries = entries * block_scale(rng, shape, cuts, -0.22, 0.18)
    return jnp.clip(entries, -limit, limit).astype(held_as)


def setup_inputs(seed: int = 0, part: int = 0) -> dict:
    keys = jax.random.split(jax.random.key(seed), 7)
    own_keys = jax.random.split(jax.random.fold_in(keys[6], part), 7)
    return {
        "hamiltonian_rows": draw_hamiltonian_rows(jax.random.fold_in(jax.random.fold_in(keys[6], part), 71), part),
        "current_block": normal_values(own_keys[1], (N, BLOCK), 1.0, 6.0, ((0, 256),), jnp.float32),
        "correction_block": normal_values(own_keys[2], (N, BLOCK), 1.0, 6.0, ((0, 256),), jnp.float32),
        "previous_block": normal_values(own_keys[3], (N, BLOCK), 1.0, 6.0, ((0, 256),), jnp.float32),
        "ritz_values": jnp.clip(jax.random.uniform(own_keys[4], (BLOCK,), jnp.float32, -2.0, 2.0), -2.0, 2.0),
        "mixing_coeffs": normal_values(own_keys[5], (3 * BLOCK, BLOCK), (3 * BLOCK) ** -0.5, 0.21875, (), jnp.float32),
    }


def matmul(left, right):
    return jnp.dot(left, right, preferred_element_type=jnp.float32, precision=lax.Precision.HIGHEST)

def tmatmul(left, right):
    return lax.dot_general(left, right, (((0,), (0,)), ((), ())), preferred_element_type=jnp.float32, precision=lax.Precision.HIGHEST)

def reference(hamiltonian_rows, current_block, correction_block, previous_block, ritz_values, mixing_coeffs):
    blocks = N_ROW * N_COL
    shard_rows = N // blocks
    whole_basis = jnp.concatenate([current_block, correction_block, previous_block], axis=1)
    window_rows = whole_basis.reshape(blocks, shard_rows, 3 * BLOCK)[:, :OUT_DEV, :].reshape(blocks * OUT_DEV, 3 * BLOCK)
    row_tile = hamiltonian_rows.reshape(blocks * OUT_DEV, N)
    product_rows = matmul(row_tile, whole_basis)
    residual = product_rows[:, :BLOCK] - window_rows[:, :BLOCK] * ritz_values[None, :]
    squares = lax.optimization_barrier(jnp.sum(residual * residual, axis=0))
    next_correction = residual * lax.rsqrt(squares / (blocks * OUT_DEV) + 1e-06)
    gram_basis = tmatmul(window_rows, window_rows)
    gram_product = tmatmul(window_rows, product_rows)
    next_block = matmul(window_rows, mixing_coeffs)
    next_direction = matmul(window_rows[:, BLOCK:], mixing_coeffs[BLOCK:, :])
    ritz_matrix = tmatmul(mixing_coeffs, matmul(gram_product, mixing_coeffs))
    metric_matrix = tmatmul(mixing_coeffs, matmul(gram_basis, mixing_coeffs))
    return (next_block, next_direction, next_correction, ritz_matrix, metric_matrix)
```

```python
import functools

import jax
import jax.numpy as jnp
from jax import lax
from jax.experimental import pallas as pl
from jax.experimental.pallas import tpu as pltpu
from jax.sharding import Mesh
from jax.sharding import PartitionSpec as P

NZ, NX = 16, 8
ROW = ("row_0", "row_1")
CHAN_ROW_COL = ("chan", "row_0", "row_1", "col")
MESH = pl.DeviceIdType.MESH
LANES = 128
HIGHEST = lax.Precision.HIGHEST


def dot(left, right):
    return jnp.dot(left, right, preferred_element_type=jnp.float32, precision=HIGHEST)


def tdot(left, right):
    return lax.dot_general(
        left,
        right,
        (((0,), (0,)), ((), ())),
        preferred_element_type=jnp.float32,
        precision=HIGHEST,
    )


def kernel(
    nz,
    nx,
    window_total,
    h_ref,
    x_ref,
    w_ref,
    p_ref,
    c_ref,
    rv_ref,
    nb_ref,
    nd_ref,
    nc_ref,
    ritz_ref,
    metric_ref,
    y_own,
    x_par,
    y_par,
    part,
    in_x,
    mid,
    in_z,
    tile,
    all_z,
    pack,
    all_x,
    nb_tile,
    nb_all_z,
    nb_pack,
    nb_all_x,
    core_own,
    core_par,
    sq_own,
    sq_par,
    xs_sem,
    xr_sem,
    zs_sem,
    zr_sem,
    azs_sem,
    azr_sem,
    axs_sem,
    axr_sem,
    nzs_sem,
    nzr_sem,
    nxs_sem,
    nxr_sem,
    cs_sem,
    cr_sem,
):
    z = lax.axis_index("row_0")
    x = lax.axis_index("row_1")
    core = lax.axis_index("col")
    other = 1 - core
    owners = nz * nx
    half = x_ref.shape[0]
    far_z = sorted(range(1, nz), key=lambda d: -min(d, nz - d))
    far_x = sorted(range(1, nx), key=lambda d: -min(d, nx - d))

    def plus_z(d):
        return lax.rem(z + d, nz)

    def plus_x(d):
        return lax.rem(x + d, nx)

    def remote(src, dst, send, recv, device):
        return pltpu.make_async_remote_copy(
            src_ref=src, dst_ref=dst, send_sem=send, recv_sem=recv, device_id=device, device_id_type=MESH
        )

    def send_z(src, dst, d, send, recv):
        copy = remote(src, dst.at[z], send.at[d], recv.at[z], {"row_0": plus_z(d)})
        copy.start()
        return copy

    def got_z(src, dst, d, send, recv):
        s = plus_z(d)
        remote(src, dst.at[s], send.at[d], recv.at[s], {"row_0": s}).wait_recv()

    def send_x(src, dst, d, send, recv):
        copy = remote(src, dst.at[x], send.at[d], recv.at[x], {"row_1": plus_x(d)})
        copy.start()
        return copy

    def got_x(src, dst, d, send, recv):
        s = plus_x(d)
        remote(src, dst.at[s], send.at[d], recv.at[s], {"row_1": s}).wait_recv()

    def core_copy(src, dst, i):
        copy = remote(src, dst, cs_sem.at[i], cr_sem.at[i], {"col": other})
        copy.start()
        return copy

    barrier = pltpu.get_barrier_semaphore()
    for d in range(1, nz):
        pl.semaphore_signal(barrier, inc=1, device_id={"row_0": plus_z(d)}, device_id_type=MESH)
    for d in range(1, nx):
        pl.semaphore_signal(barrier, inc=1, device_id={"row_1": plus_x(d)}, device_id_type=MESH)
    pl.semaphore_signal(barrier, inc=1, device_id={"col": other}, device_id_type=MESH)

    direction = dot(w_ref[...], c_ref[half : 2 * half, :]) + dot(p_ref[...], c_ref[2 * half :, :])
    nd_ref[...] = direction[:2, :]
    y_own[...] = direction + dot(x_ref[...], c_ref[:half, :])
    nb_ref[...] = y_own[0:2, :]
    nb_tile[...] = jnp.zeros_like(nb_tile)
    for j in range(2):
        for q in range(2):
            nb_tile[j * 4 + q : j * 4 + q + 1, :] = y_own[j : j + 1, q * LANES : (q + 1) * LANES]

    pl.semaphore_wait(barrier, nz + nx - 1)

    copies = []
    x_core = core_copy(x_ref, x_par, 0)
    y_core = core_copy(y_own, y_par, 1)
    for d in far_z:
        copies.append(send_z(nb_tile, nb_all_z, d, nzs_sem, nzr_sem))

    def h_cols(which):
        tiles = half // LANES
        rows = []
        for j in range(2):
            rows.append(
                jnp.concatenate(
                    [h_ref[pl.ds((which * tiles + t) * 2 + j, owners, stride=8), :] for t in range(tiles)], axis=1
                )
            )
        return jnp.concatenate(rows, axis=0)

    def put(value, first):
        for j in range(2):
            for q in range(2):
                block = value[j * owners : (j + 1) * owners, q * LANES : (q + 1) * LANES]
                part[:, :, j * 4 + first + q, :] = block.reshape(nz, nx, LANES)

    h_own = h_cols(core)
    h_par = h_cols(other)
    hx = dot(h_own, x_ref[...])
    hy = dot(h_own, y_own[...])
    x_core.wait_recv()
    put(hx + dot(h_par, x_par[...]), 0)
    y_core.wait_recv()
    put(hy + dot(h_par, y_par[...]), 2)

    for d in far_x:
        copies.append(send_x(part.at[:, plus_x(d)], in_x, d, xs_sem, xr_sem))

    def repack(source, first, packed):
        for j in range(2):
            for q in range(2):
                packed[(j * 2 + q) * nz : (j * 2 + q + 1) * nz, :] = source[:, j * 4 + first + q, :]

    nb_all_z[z] = nb_tile[...]
    for d in range(1, nz):
        got_z(nb_tile, nb_all_z, d, nzs_sem, nzr_sem)
    repack(nb_all_z, 0, nb_pack)
    nb_all_x[x] = nb_pack[...]
    for d in far_x:
        copies.append(send_x(nb_pack, nb_all_x, d, nxs_sem, nxr_sem))

    for d in range(1, nx):
        got_x(part.at[:, x], in_x, d, xs_sem, xr_sem)
    total = part[:, x]
    for d in range(1, nx):
        total = total + in_x[plus_x(d)]
    mid[...] = total

    for d in far_z:
        copies.append(send_z(mid.at[plus_z(d)], in_z, d, zs_sem, zr_sem))
    own_sum = mid[z]
    for d in range(1, nz):
        got_z(mid.at[z], in_z, d, zs_sem, zr_sem)
    for d in range(1, nz):
        own_sum = own_sum + in_z[plus_z(d)]
    tile[...] = own_sum

    residual = []
    for j in range(2):
        residual.append(
            [
                tile[j * 4 + q : j * 4 + q + 1, :]
                - x_ref[j : j + 1, q * LANES : (q + 1) * LANES] * rv_ref[:, q * LANES : (q + 1) * LANES]
                for q in range(2)
            ]
        )
    for q in range(2):
        tile[q : q + 1, :] = residual[0][q] * residual[0][q] + residual[1][q] * residual[1][q]

    for d in far_z:
        copies.append(send_z(tile, all_z, d, azs_sem, azr_sem))
    all_z[z] = tile[...]
    for d in range(1, nz):
        got_z(tile, all_z, d, azs_sem, azr_sem)
    repack(all_z, 2, pack)
    pack[4 * nz :, :] = jnp.zeros((8, LANES), jnp.float32)
    for q in range(2):
        pack[4 * nz + q : 4 * nz + q + 1, :] = jnp.sum(all_z[:, q, :], axis=0, keepdims=True)
    for d in far_x:
        copies.append(send_x(pack, all_x, d, axs_sem, axr_sem))
    all_x[x] = pack[...]

    def rows_of(source):
        columns = []
        for q in range(2):
            columns.append(
                jnp.concatenate(
                    [source[:, (j * 2 + q) * nz : (j * 2 + q + 1) * nz, :].reshape(owners, LANES) for j in range(2)],
                    axis=0,
                )
            )
        return jnp.concatenate(columns, axis=1)

    for d in range(1, nx):
        got_x(nb_pack, nb_all_x, d, nxs_sem, nxr_sem)
    nb_rows = rows_of(nb_all_x)
    core_own[0] = tdot(nb_rows, nb_rows)
    metric_core = core_copy(core_own.at[0], core_par.at[0], 2)

    for d in range(1, nx):
        got_x(pack, all_x, d, axs_sem, axr_sem)
    sq_own[...] = jnp.sum(all_x[:, 4 * nz :, :], axis=0)
    sq_core = core_copy(sq_own, sq_par, 3)
    core_own[1] = tdot(nb_rows, rows_of(all_x))
    ritz_core = core_copy(core_own.at[1], core_par.at[1], 4)

    metric_core.wait_recv()
    metric_ref[...] = core_own[0] + core_par[0]
    sq_core.wait_recv()
    squares = sq_own[...] + sq_par[...]
    for q in range(2):
        scale = lax.rsqrt(squares[q : q + 1, :] / window_total + 1e-06)
        for j in range(2):
            nc_ref[j : j + 1, q * LANES : (q + 1) * LANES] = residual[j][q] * scale
    ritz_core.wait_recv()
    ritz_ref[...] = core_own[1] + core_par[1]

    for copy in copies + [x_core, y_core, metric_core, sq_core, ritz_core]:
        copy.wait_send()


def on_device(hamiltonian_rows, current_block, correction_block, previous_block, ritz_values, mixing_coeffs):
    nz, nx = lax.axis_size("row_0"), lax.axis_size("row_1")
    owners, _, out_rows, columns = hamiltonian_rows.shape
    block_width = current_block.shape[1]
    window_total = out_rows * owners * lax.axis_size("col")
    tiles = columns // LANES
    h_flat = hamiltonian_rows.reshape(owners, out_rows, tiles, LANES).transpose(0, 2, 1, 3)
    h_flat = h_flat.reshape(owners * tiles * out_rows, LANES)
    f32 = functools.partial(jax.ShapeDtypeStruct, dtype=jnp.float32)
    vmem = pl.BlockSpec(memory_space=pltpu.VMEM)
    square = (block_width, block_width)

    def buffer(*shape):
        return pltpu.VMEM(shape, jnp.float32)

    sems = pltpu.SemaphoreType.DMA
    sem_sizes = (nx, nx, nz, nz, nz, nz, nx, nx, nz, nz, nx, nx, 5, 5)
    return pl.pallas_call(
        functools.partial(kernel, nz, nx, window_total),
        out_shape=(
            f32((out_rows, block_width)),
            f32((out_rows, block_width)),
            f32((out_rows, block_width)),
            f32(square),
            f32(square),
        ),
        in_specs=[vmem] * 6,
        out_specs=(vmem,) * 5,
        scratch_shapes=[
            buffer(*square),
            buffer(*square),
            buffer(*square),
            buffer(nz, nx, 8, LANES),
            buffer(nx, nz, 8, LANES),
            buffer(nz, 8, LANES),
            buffer(nz, 8, LANES),
            buffer(8, LANES),
            buffer(nz, 8, LANES),
            buffer(4 * nz + 8, LANES),
            buffer(nx, 4 * nz + 8, LANES),
            buffer(8, LANES),
            buffer(nz, 8, LANES),
            buffer(4 * nz, LANES),
            buffer(nx, 4 * nz, LANES),
            buffer(2, *square),
            buffer(2, *square),
            buffer(8, LANES),
            buffer(8, LANES),
        ]
        + [sems((n,)) for n in sem_sizes],
        compiler_params=pltpu.CompilerParams(collective_id=0, has_side_effects=True),
        name="lobpcg_step",
    )(h_flat, current_block, correction_block, previous_block, mixing_coeffs, ritz_values.reshape(1, -1))


def solution(mesh):
    finer = Mesh(
        mesh.devices.reshape(mesh.shape["chan"], NZ, NX, mesh.shape["col"]),
        ("chan", "row_0", "row_1", "col"),
    )
    in_specs = (
        P("chan", "col", None, ROW),
        P(CHAN_ROW_COL, None),
        P(CHAN_ROW_COL, None),
        P(CHAN_ROW_COL, None),
        P("chan"),
        P("chan", None),
    )
    out_specs = (
        P(CHAN_ROW_COL, None),
        P(CHAN_ROW_COL, None),
        P(CHAN_ROW_COL, None),
        P("chan", None),
        P("chan", None),
    )
    return jax.shard_map(on_device, mesh=finer, in_specs=in_specs, out_specs=out_specs, check_vma=False)
```

```python
import functools

import jax
import jax.numpy as jnp
from jax import lax
from jax.experimental import pallas as pl
from jax.experimental.pallas import tpu as pltpu
from jax.sharding import Mesh
from jax.sharding import PartitionSpec as P

NZ, NX = 16, 8
ROW = ("row_0", "row_1")
CHAN_ROW_COL = ("chan", "row_0", "row_1", "col")
MESH = pl.DeviceIdType.MESH
LANES = 128
MAIN_VMEM = 24 * 2**20
END_VMEM = 8 * 2**20
HIGHEST = lax.Precision.HIGHEST


def dot(left, right):
    return jnp.dot(left, right, preferred_element_type=jnp.float32, precision=HIGHEST)


def tdot(left, right):
    return lax.dot_general(
        left,
        right,
        (((0,), (0,)), ((), ())),
        preferred_element_type=jnp.float32,
        precision=HIGHEST,
    )


def kernel(
    nz,
    nx,
    h_hbm,
    x_hbm,
    w_hbm,
    p_hbm,
    c_hbm,
    rv_hbm,
    small_ref,
    ritz_ref,
    metric_ref,
    rv_ref,
    h_ref,
    x_ref,
    w_ref,
    p_ref,
    c_ref,
    y_own,
    x_par,
    y_par,
    part,
    in_x,
    mid,
    in_z,
    tile,
    all_z,
    pack,
    all_x,
    sq_tile,
    sq_all,
    nb_tile,
    nb_all_z,
    nb_pack,
    nb_all_x,
    core_own,
    core_par,
    sq_own,
    sq_par,
    in_sem,
    xs_sem,
    xr_sem,
    zs_sem,
    zr_sem,
    azs_sem,
    azr_sem,
    axs_sem,
    axr_sem,
    qs_sem,
    qr_sem,
    nzs_sem,
    nzr_sem,
    nxs_sem,
    nxr_sem,
    cs_sem,
    cr_sem,
):
    z = lax.axis_index("row_0")
    x = lax.axis_index("row_1")
    core = lax.axis_index("col")
    other = 1 - core
    owners = nz * nx
    pairs = nz // 2
    half = x_ref.shape[0]
    own_pair = z // 2
    z_mate = 2 * own_pair + 1 - lax.rem(z, 2)
    far_z = sorted(range(1, nz), key=lambda d: -min(d, nz - d))
    far_x = sorted(range(1, nx), key=lambda d: -min(d, nx - d))
    far_pairs = sorted(range(pairs), key=lambda k: -min(k, pairs - k))
    near_pairs = far_pairs[::-1]

    def plus_z(d):
        return lax.rem(z + d, nz)

    def plus_x(d):
        return lax.rem(x + d, nx)

    def pair_at(k):
        return lax.rem(own_pair + k, pairs)

    def remote(src, dst, send, recv, device):
        return pltpu.make_async_remote_copy(
            src_ref=src, dst_ref=dst, send_sem=send, recv_sem=recv, device_id=device, device_id_type=MESH
        )

    copies = []

    def send(src, dst, send_sem, recv_sem, device):
        copy = remote(src, dst, send_sem, recv_sem, device)
        copy.start()
        copies.append(copy)
        return copy

    def got(dst, send_sem, recv_sem, device):
        remote(dst, dst, send_sem, recv_sem, device).wait_recv()

    loads = []
    for i, (src, dst) in enumerate(
        [(w_hbm, w_ref), (c_hbm, c_ref), (p_hbm, p_ref), (x_hbm, x_ref), (h_hbm, h_ref), (rv_hbm, rv_ref)]
    ):
        loads.append(pltpu.make_async_copy(src, dst, in_sem.at[i]))
        loads[i].start()

    barrier = pltpu.get_barrier_semaphore()
    for d in far_z:
        pl.semaphore_signal(barrier, inc=1, device_id={"row_0": plus_z(d)}, device_id_type=MESH)
    for d in far_x:
        pl.semaphore_signal(barrier, inc=1, device_id={"row_1": plus_x(d)}, device_id_type=MESH)
    pl.semaphore_signal(barrier, inc=1, device_id={"col": other}, device_id_type=MESH)

    loads[0].wait()
    loads[1].wait()
    direction = dot(w_ref[...], c_ref[half : 2 * half, :])
    loads[2].wait()
    direction = direction + dot(p_ref[...], c_ref[2 * half :, :])
    small_ref[2:4, :] = direction[:2, :]
    loads[3].wait()
    y_own[...] = direction + dot(x_ref[...], c_ref[:half, :])
    small_ref[0:2, :] = y_own[0:2, :]
    nb_tile[...] = jnp.zeros_like(nb_tile)
    for j in range(2):
        for q in range(2):
            row = 4 + j * 2 + q
            nb_tile[row : row + 1, :] = y_own[j : j + 1, q * LANES : (q + 1) * LANES]

    pl.semaphore_wait(barrier, nz + nx - 1)

    x_core = send(x_ref, x_par, cs_sem.at[0], cr_sem.at[0], {"col": other})
    y_core = send(y_own, y_par, cs_sem.at[1], cr_sem.at[1], {"col": other})
    for d in far_z:
        send(nb_tile, nb_all_z.at[z], nzs_sem.at[d], nzr_sem.at[z], {"row_0": plus_z(d)})

    def h_cols(which):
        tiles = half // LANES
        rows = []
        for j in range(2):
            rows.append(
                jnp.concatenate(
                    [h_ref[pl.ds((which * tiles + t) * 2 + j, owners, stride=8), :] for t in range(tiles)], axis=1
                )
            )
        return jnp.concatenate(rows, axis=0)

    def put(value, which):
        for j in range(2):
            for q in range(2):
                block = value[j * owners : (j + 1) * owners, q * LANES : (q + 1) * LANES]
                part[:, :, which * 4 + j * 2 + q, :] = block.reshape(nz, nx, LANES)

    loads[4].wait()
    loads[5].wait()
    h_own = h_cols(core)
    h_par = h_cols(other)
    hx = dot(h_own, x_ref[...])
    hy = dot(h_own, y_own[...])
    x_core.wait_recv()
    put(hx + dot(h_par, x_par[...]), 0)
    y_core.wait_recv()
    put(hy + dot(h_par, y_par[...]), 1)

    for k in far_pairs:
        first = 2 * pair_at(k)
        for d in far_x:
            send(
                part.at[pl.ds(first, 2), plus_x(d)],
                in_x.at[x, pl.ds(first, 2)],
                xs_sem.at[d, k],
                xr_sem.at[x, pair_at(k)],
                {"row_1": plus_x(d)},
            )

    def pack_pair(source, packed, pair):
        for low in range(2):
            packed[pair, low * 4 : (low + 1) * 4, :] = source[2 * pair + low, 4:8, :]

    nb_all_z[z] = nb_tile[...]
    for d in range(1, nz):
        s = plus_z(d)
        got(nb_all_z.at[s], nzs_sem.at[d], nzr_sem.at[s], {"row_0": s})
    for pair in range(pairs):
        pack_pair(nb_all_z, nb_pack, pair)
    nb_all_x[x] = nb_pack[...]
    for d in far_x:
        send(nb_pack, nb_all_x.at[x], nxs_sem.at[d], nxr_sem.at[x], {"row_1": plus_x(d)})

    for k in far_pairs:
        pair = pair_at(k)
        first = 2 * pair
        for d in range(1, nx):
            s = plus_x(d)
            got(in_x.at[s, pl.ds(first, 2)], xs_sem.at[d, k], xr_sem.at[s, pair], {"row_1": s})
        total = part[pl.ds(first, 2), x]
        for d in range(1, nx):
            total = total + in_x[plus_x(d), pl.ds(first, 2)]
        mid[pl.ds(first, 2)] = total
        if k:
            for low in range(2):
                to = first + low
                send(mid.at[to], in_z.at[z], zs_sem.at[2 * k + low], zr_sem.at[z], {"row_0": to})
        else:
            send(mid.at[z_mate], in_z.at[z], zs_sem.at[0], zr_sem.at[z], {"row_0": z_mate})

    own_sum = mid[z]
    for d in far_z:
        s = plus_z(d)
        got(in_z.at[s], zs_sem.at[d], zr_sem.at[s], {"row_0": s})
    for d in far_z:
        own_sum = own_sum + in_z[plus_z(d)]
    tile[...] = own_sum

    for q in range(2):
        squares = 0.0
        for j in range(2):
            columns = slice(q * LANES, (q + 1) * LANES)
            residual = tile[j * 2 + q : j * 2 + q + 1, :] - x_ref[j : j + 1, columns] * rv_ref[:, columns]
            small_ref[4 + j : 5 + j, columns] = residual
            squares = squares + residual * residual
        sq_own[q : q + 1, :] = squares
    tile[0:2, :] = sq_own[0:2, :]

    for d in far_z:
        send(tile, all_z.at[z], azs_sem.at[d], azr_sem.at[z], {"row_0": plus_z(d)})
    all_z[z] = tile[...]
    for k in near_pairs:
        pair = pair_at(k)
        for s in [2 * pair, 2 * pair + 1] if k else [z_mate]:
            got(all_z.at[s], azs_sem.at[0], azr_sem.at[s], {"row_0": s})
        pack_pair(all_z, pack, pair)
        for d in far_x:
            send(pack.at[pair], all_x.at[x, pair], axs_sem.at[d, k], axr_sem.at[x, pair], {"row_1": plus_x(d)})
    all_x[x] = pack[...]
    sq_tile[...] = jnp.sum(all_z[...], axis=0)
    for d in far_x:
        send(sq_tile, sq_all.at[x], qs_sem.at[d], qr_sem.at[x], {"row_1": plus_x(d)})
    sq_all[x] = sq_tile[...]

    def rows_of(source):
        columns = []
        for q in range(2):
            columns.append(
                jnp.concatenate(
                    [source[:, :, 2 * i + q, :].reshape(nx * pairs, LANES) for i in range(4)],
                    axis=0,
                )
            )
        return jnp.concatenate(columns, axis=1)

    for d in range(1, nx):
        s = plus_x(d)
        got(nb_all_x.at[s], nxs_sem.at[d], nxr_sem.at[s], {"row_1": s})
    nb_rows = rows_of(nb_all_x)
    core_own[0] = tdot(nb_rows, nb_rows)
    metric_core = send(core_own.at[0], core_par.at[0], cs_sem.at[2], cr_sem.at[2], {"col": other})

    for k in near_pairs:
        pair = pair_at(k)
        for d in range(1, nx):
            s = plus_x(d)
            got(all_x.at[s, pair], axs_sem.at[d, k], axr_sem.at[s, pair], {"row_1": s})
    core_own[1] = tdot(nb_rows, rows_of(all_x))
    ritz_core = send(core_own.at[1], core_par.at[1], cs_sem.at[4], cr_sem.at[4], {"col": other})

    for d in range(1, nx):
        s = plus_x(d)
        got(sq_all.at[s], qs_sem.at[d], qr_sem.at[s], {"row_1": s})
    sq_own[...] = jnp.sum(sq_all[...], axis=0)
    sq_core = send(sq_own, sq_par, cs_sem.at[3], cr_sem.at[3], {"col": other})
    metric_core.wait_recv()
    metric_ref[...] = core_own[0] + core_par[0]
    sq_core.wait_recv()
    for q in range(2):
        small_ref[6:7, q * LANES : (q + 1) * LANES] = sq_own[q : q + 1, :] + sq_par[q : q + 1, :]
    small_ref[7:8, :] = jnp.zeros((1, small_ref.shape[1]), jnp.float32)
    ritz_core.wait_recv()
    ritz_ref[...] = core_own[1] + core_par[1]

    for copy in copies:
        copy.wait_send()


def finish(window_total, small_in, ritz_in, metric_in, nb_ref, nd_ref, nc_ref, ritz_ref, metric_ref):
    ritz_ref[...] = ritz_in[...]
    metric_ref[...] = metric_in[...]
    nb_ref[...] = small_in[0:2, :]
    nd_ref[...] = small_in[2:4, :]
    nc_ref[...] = small_in[4:6, :] * lax.rsqrt(small_in[6:7, :] / window_total + 1e-06)


def on_device(hamiltonian_rows, current_block, correction_block, previous_block, ritz_values, mixing_coeffs):
    nz, nx = lax.axis_size("row_0"), lax.axis_size("row_1")
    pairs = nz // 2
    owners, _, out_rows, columns = hamiltonian_rows.shape
    block_width = current_block.shape[1]
    window_total = out_rows * owners * lax.axis_size("col")
    tiles = columns // LANES
    h_flat = hamiltonian_rows.reshape(owners, out_rows, tiles, LANES).transpose(0, 2, 1, 3)
    h_flat = h_flat.reshape(owners * tiles * out_rows, LANES)
    f32 = functools.partial(jax.ShapeDtypeStruct, dtype=jnp.float32)
    vmem = pl.BlockSpec(memory_space=pltpu.VMEM)
    hbm = pl.BlockSpec(memory_space=pltpu.HBM)
    square = (block_width, block_width)

    def buffer(*shape):
        return pltpu.VMEM(shape, jnp.float32)

    sems = pltpu.SemaphoreType.DMA
    sem_shapes = [
        (6,),
        (nx, pairs),
        (nx, pairs),
        (nz,),
        (nz,),
        (nz,),
        (nz,),
        (nx, pairs),
        (nx, pairs),
        (nx,),
        (nx,),
        (nz,),
        (nz,),
        (nx,),
        (nx,),
        (5,),
        (5,),
    ]
    small, ritz, metric = pl.pallas_call(
        functools.partial(kernel, nz, nx),
        out_shape=(f32((8, block_width)), f32(square), f32(square)),
        in_specs=[hbm] * 6,
        out_specs=(vmem,) * 3,
        scratch_shapes=[
            buffer(1, block_width),
            buffer(*h_flat.shape),
            buffer(*square),
            buffer(*square),
            buffer(*square),
            buffer(*mixing_coeffs.shape),
            buffer(*square),
            buffer(*square),
            buffer(*square),
            buffer(nz, nx, 8, LANES),
            buffer(nx, nz, 8, LANES),
            buffer(nz, 8, LANES),
            buffer(nz, 8, LANES),
            buffer(8, LANES),
            buffer(nz, 8, LANES),
            buffer(pairs, 8, LANES),
            buffer(nx, pairs, 8, LANES),
            buffer(8, LANES),
            buffer(nx, 8, LANES),
            buffer(8, LANES),
            buffer(nz, 8, LANES),
            buffer(pairs, 8, LANES),
            buffer(nx, pairs, 8, LANES),
            buffer(2, *square),
            buffer(2, *square),
            buffer(8, LANES),
            buffer(8, LANES),
        ]
        + [sems(shape) for shape in sem_shapes],
        compiler_params=pltpu.CompilerParams(
            collective_id=0, has_side_effects=True, vmem_limit_bytes=MAIN_VMEM
        ),
        name="lobpcg_step",
    )(
        *(
            pltpu.with_memory_space_constraint(a, pltpu.HBM)
            for a in (
                h_flat,
                current_block,
                correction_block,
                previous_block,
                mixing_coeffs,
                ritz_values.reshape(1, -1),
            )
        )
    )
    return pl.pallas_call(
        functools.partial(finish, window_total),
        out_shape=(f32((out_rows, block_width)),) * 3 + (f32(square),) * 2,
        in_specs=[vmem] * 3,
        out_specs=(vmem,) * 5,
        compiler_params=pltpu.CompilerParams(vmem_limit_bytes=END_VMEM),
        name="finish",
    )(small, ritz, metric)


def solution(mesh):
    finer = Mesh(
        mesh.devices.reshape(mesh.shape["chan"], NZ, NX, mesh.shape["col"]),
        ("chan", "row_0", "row_1", "col"),
    )
    in_specs = (
        P("chan", "col", None, ROW),
        P(CHAN_ROW_COL, None),
        P(CHAN_ROW_COL, None),
        P(CHAN_ROW_COL, None),
        P("chan"),
        P("chan", None),
    )
    out_specs = (
        P(CHAN_ROW_COL, None),
        P(CHAN_ROW_COL, None),
        P(CHAN_ROW_COL, None),
        P("chan", None),
        P("chan", None),
    )
    return jax.shard_map(on_device, mesh=finer, in_specs=in_specs, out_specs=out_specs, check_vma=False)
```

```python
import functools

import jax
import jax.numpy as jnp
from jax import lax
from jax.experimental import pallas as pl
from jax.experimental.pallas import tpu as pltpu
from jax.sharding import Mesh
from jax.sharding import PartitionSpec as P

NZ, NX = 16, 8
ROW = ("row_0", "row_1")
CHAN_ROW_COL = ("chan", "row_0", "row_1", "col")
MESH = pl.DeviceIdType.MESH
LANES = 128
MAIN_VMEM = 24 * 2**20
END_VMEM = 8 * 2**20
HIGHEST = lax.Precision.HIGHEST


def dot(left, right):
    return jnp.dot(left, right, preferred_element_type=jnp.float32, precision=HIGHEST)


def tdot(left, right):
    return lax.dot_general(
        left,
        right,
        (((0,), (0,)), ((), ())),
        preferred_element_type=jnp.float32,
        precision=HIGHEST,
    )


def kernel(
    nz,
    nx,
    h_hbm,
    x_hbm,
    w_hbm,
    p_hbm,
    c_hbm,
    rv_hbm,
    small_ref,
    ritz_ref,
    metric_ref,
    rv_ref,
    h_ref,
    x_ref,
    w_ref,
    p_ref,
    c_ref,
    y_own,
    x_par,
    y_par,
    part_x,
    part_y,
    in_x,
    in_y,
    hop_in_x,
    hop_in_y,
    hop_x,
    hop_y,
    mid_x,
    mid_y,
    in_xz,
    in_yz,
    tile_x,
    tile_y,
    y_all_z,
    y_all_x,
    sq_tile,
    sq_all_z,
    sq_sum,
    sq_all_x,
    nb_tile,
    nb_all_z,
    nb_all_x,
    core_own,
    core_par,
    sq_own,
    sq_par,
    in_sem,
    xs_sem,
    xr_sem,
    ys_sem,
    yr_sem,
    hxs_sem,
    hxr_sem,
    hys_sem,
    hyr_sem,
    xzs_sem,
    xzr_sem,
    yzs_sem,
    yzr_sem,
    gzs_sem,
    gzr_sem,
    gxs_sem,
    gxr_sem,
    qzs_sem,
    qzr_sem,
    qxs_sem,
    qxr_sem,
    nzs_sem,
    nzr_sem,
    nxs_sem,
    nxr_sem,
    cs_sem,
    cr_sem,
):
    z = lax.axis_index("row_0")
    x = lax.axis_index("row_1")
    core = lax.axis_index("col")
    other = 1 - core
    owners = nz * nx
    pairs = nz // 2
    half = x_ref.shape[0]
    opposite = nx // 2
    own_pair = z // 2
    z_mate = 2 * own_pair + 1 - lax.rem(z, 2)
    far_z = sorted(range(1, nz), key=lambda d: -min(d, nz - d))
    far_x = sorted(range(1, nx), key=lambda d: -min(d, nx - d))
    near_x = [d for d in far_x if d != opposite]
    far_pairs = sorted(range(pairs), key=lambda k: -min(k, pairs - k))
    near_pairs = far_pairs[::-1]

    def plus_z(d):
        return lax.rem(z + d, nz)

    def plus_x(d):
        return lax.rem(x + d % nx, nx)

    def pair_at(k):
        return lax.rem(own_pair + k, pairs)

    def way(k):
        return 1 if k % 2 == 0 else -1

    def remote(src, dst, send, recv, device):
        return pltpu.make_async_remote_copy(
            src_ref=src, dst_ref=dst, send_sem=send, recv_sem=recv, device_id=device, device_id_type=MESH
        )

    copies = []

    def send(src, dst, send_sem, recv_sem, device):
        copy = remote(src, dst, send_sem, recv_sem, device)
        copy.start()
        copies.append(copy)
        return copy

    def got(dst, send_sem, recv_sem, device):
        remote(dst, dst, send_sem, recv_sem, device).wait_recv()

    loads = []
    for i, (src, dst) in enumerate(
        [(w_hbm, w_ref), (c_hbm, c_ref), (p_hbm, p_ref), (x_hbm, x_ref), (h_hbm, h_ref), (rv_hbm, rv_ref)]
    ):
        loads.append(pltpu.make_async_copy(src, dst, in_sem.at[i]))
        loads[i].start()

    barrier = pltpu.get_barrier_semaphore()
    for d in far_z:
        pl.semaphore_signal(barrier, inc=1, device_id={"row_0": plus_z(d)}, device_id_type=MESH)
    for d in far_x:
        pl.semaphore_signal(barrier, inc=1, device_id={"row_1": plus_x(d)}, device_id_type=MESH)
    pl.semaphore_signal(barrier, inc=1, device_id={"col": other}, device_id_type=MESH)

    loads[0].wait()
    loads[1].wait()
    direction = dot(w_ref[...], c_ref[half : 2 * half, :])
    loads[2].wait()
    direction = direction + dot(p_ref[...], c_ref[2 * half :, :])
    small_ref[2:4, :] = direction[:2, :]
    loads[3].wait()
    y_own[...] = direction + dot(x_ref[...], c_ref[:half, :])
    small_ref[0:2, :] = y_own[0:2, :]
    for j in range(2):
        for q in range(2):
            nb_tile[j * 2 + q : j * 2 + q + 1, :] = y_own[j : j + 1, q * LANES : (q + 1) * LANES]

    pl.semaphore_wait(barrier, nz + nx - 1)

    y_core = send(y_own, y_par, cs_sem.at[1], cr_sem.at[1], {"col": other})
    x_core = send(x_ref, x_par, cs_sem.at[0], cr_sem.at[0], {"col": other})
    for d in far_z:
        send(nb_tile, nb_all_z.at[z], nzs_sem.at[d], nzr_sem.at[z], {"row_0": plus_z(d)})

    def h_cols(which):
        tiles = half // LANES
        rows = []
        for j in range(2):
            rows.append(
                jnp.concatenate(
                    [h_ref[pl.ds((which * tiles + t) * 2 + j, owners, stride=8), :] for t in range(tiles)], axis=1
                )
            )
        return jnp.concatenate(rows, axis=0)

    def put(value, part):
        for j in range(2):
            for q in range(2):
                block = value[j * owners : (j + 1) * owners, q * LANES : (q + 1) * LANES]
                part[:, :, j * 2 + q, :] = block.reshape(nz, nx, LANES)

    def send_chunk(part, into, s_sem, r_sem, k, d):
        pair = pair_at(k)
        send(
            part.at[pl.ds(2 * pair, 2), plus_x(d)],
            into.at[x, pl.ds(2 * pair, 2)],
            s_sem.at[d % nx, k],
            r_sem.at[x, pair],
            {"row_1": plus_x(d)},
        )

    def start_sum(part, into, s_sem, r_sem, hop_in, hs_sem, hr_sem):
        for k in far_pairs:
            send(
                part.at[pl.ds(2 * pair_at(k), 2), plus_x(opposite)],
                hop_in.at[k],
                hs_sem.at[k],
                hr_sem.at[k],
                {"row_1": plus_x(way(k))},
            )
        for k in far_pairs:
            for d in near_x:
                if d != way(k) * (opposite - 1) % nx:
                    send_chunk(part, into, s_sem, r_sem, k, d)

    def hop_on(part, into, s_sem, r_sem, hop_in, hop, hs_sem, hr_sem):
        for k in far_pairs:
            pair = pair_at(k)
            d = way(k) * (opposite - 1)
            got(hop_in.at[k], hs_sem.at[k], hr_sem.at[k], {"row_1": plus_x(-way(k))})
            hop[k] = hop_in[k] + part[pl.ds(2 * pair, 2), plus_x(d)]
            send(
                hop.at[k],
                into.at[x, pl.ds(2 * pair, 2)],
                s_sem.at[d % nx, k],
                r_sem.at[x, pair],
                {"row_1": plus_x(d)},
            )

    def sum_pairs(part, into, s_sem, r_sem, mid, into_z, zs_sem, zr_sem):
        for k in far_pairs:
            pair = pair_at(k)
            first = 2 * pair
            for d in near_x:
                s = plus_x(d)
                got(into.at[s, pl.ds(first, 2)], s_sem.at[d, k], r_sem.at[s, pair], {"row_1": s})
            total = part[pl.ds(first, 2), x]
            for d in near_x:
                total = total + into[plus_x(d), pl.ds(first, 2)]
            mid[pl.ds(first, 2)] = total
            if k:
                for low in range(2):
                    to = first + low
                    send(mid.at[to], into_z.at[z], zs_sem.at[2 * k + low], zr_sem.at[z], {"row_0": to})
            else:
                send(mid.at[z_mate], into_z.at[z], zs_sem.at[0], zr_sem.at[z], {"row_0": z_mate})

    def sum_z(mid, into_z, zs_sem, zr_sem):
        for d in far_z:
            s = plus_z(d)
            got(into_z.at[s], zs_sem.at[d], zr_sem.at[s], {"row_0": s})
        total = mid[z]
        for d in far_z:
            total = total + into_z[plus_z(d)]
        return total

    y_sum = (part_y, in_y, ys_sem, yr_sem)
    x_sum = (part_x, in_x, xs_sem, xr_sem)
    loads[4].wait()
    loads[5].wait()
    h_own = h_cols(core)
    h_par = h_cols(other)
    hy = dot(h_own, y_own[...])
    y_core.wait_recv()
    put(hy + dot(h_par, y_par[...]), part_y)
    start_sum(*y_sum, hop_in_y, hys_sem, hyr_sem)
    hx = dot(h_own, x_ref[...])
    x_core.wait_recv()
    put(hx + dot(h_par, x_par[...]), part_x)
    hop_on(*y_sum, hop_in_y, hop_y, hys_sem, hyr_sem)
    start_sum(*x_sum, hop_in_x, hxs_sem, hxr_sem)
    sum_pairs(*y_sum, mid_y, in_yz, yzs_sem, yzr_sem)
    hop_on(*x_sum, hop_in_x, hop_x, hxs_sem, hxr_sem)

    tile_y[...] = sum_z(mid_y, in_yz, yzs_sem, yzr_sem)
    for d in far_z:
        send(tile_y, y_all_z.at[z], gzs_sem.at[d], gzr_sem.at[z], {"row_0": plus_z(d)})
    y_all_z[z] = tile_y[...]

    def ring(step):
        for sign in (1, -1):
            if step <= opposite - (sign < 0):
                s = plus_x(-sign * (step - 1))
                slot = sign * step % nx
                if step > 1:
                    got(nb_all_x.at[s], nxs_sem.at[slot], nxr_sem.at[s], {"row_1": s})
                send(
                    nb_all_x.at[s] if step > 1 else nb_all_z,
                    nb_all_x.at[s],
                    nxs_sem.at[slot],
                    nxr_sem.at[s],
                    {"row_1": plus_x(sign)},
                )

    nb_all_z[z] = nb_tile[...]
    for d in range(1, nz):
        s = plus_z(d)
        got(nb_all_z.at[s], nzs_sem.at[d], nzr_sem.at[s], {"row_0": s})
    ring(1)
    nb_all_x[x] = nb_all_z[...]

    sum_pairs(*x_sum, mid_x, in_xz, xzs_sem, xzr_sem)
    ring(2)
    tile_x[...] = sum_z(mid_x, in_xz, xzs_sem, xzr_sem)
    for q in range(2):
        squares = 0.0
        for j in range(2):
            columns = slice(q * LANES, (q + 1) * LANES)
            residual = tile_x[j * 2 + q : j * 2 + q + 1, :] - x_ref[j : j + 1, columns] * rv_ref[:, columns]
            small_ref[4 + j : 5 + j, columns] = residual
            squares = squares + residual * residual
        sq_tile[q : q + 1, :] = squares
    for d in far_z:
        send(sq_tile, sq_all_z.at[z], qzs_sem.at[d], qzr_sem.at[z], {"row_0": plus_z(d)})
    sq_all_z[z] = sq_tile[...]
    ring(3)

    for k in near_pairs:
        pair = pair_at(k)
        for s in [2 * pair, 2 * pair + 1] if k else [z_mate]:
            got(y_all_z.at[s], gzs_sem.at[0], gzr_sem.at[s], {"row_0": s})
        pair_slice = pl.ds(2 * pair, 2)
        for d in far_x:
            send(
                y_all_z.at[pair_slice],
                y_all_x.at[x, pair_slice],
                gxs_sem.at[d, k],
                gxr_sem.at[x, pair],
                {"row_1": plus_x(d)},
            )
    y_all_x[x] = y_all_z[...]

    def rows_of(source):
        columns = []
        for q in range(2):
            columns.append(
                jnp.concatenate([source[:, :, 2 * j + q, :].reshape(owners, LANES) for j in range(2)], axis=0)
            )
        return jnp.concatenate(columns, axis=1)

    for step in range(4, opposite + 1):
        ring(step)
    ends = {opposite, 1 - opposite} if opposite > 1 else {1}
    for d in sorted(ends):
        s = plus_x(-d)
        got(nb_all_x.at[s], nxs_sem.at[0], nxr_sem.at[s], {"row_1": s})
    nb_rows = rows_of(nb_all_x)
    core_own[0] = tdot(nb_rows, nb_rows)
    metric_core = send(core_own.at[0], core_par.at[0], cs_sem.at[2], cr_sem.at[2], {"col": other})

    for d in far_z:
        s = plus_z(d)
        got(sq_all_z.at[s], qzs_sem.at[d], qzr_sem.at[s], {"row_0": s})
    sq_sum[...] = jnp.sum(sq_all_z[...], axis=0)
    for d in far_x:
        send(sq_sum, sq_all_x.at[x], qxs_sem.at[d], qxr_sem.at[x], {"row_1": plus_x(d)})
    sq_all_x[x] = sq_sum[...]

    for k in near_pairs:
        pair = pair_at(k)
        for d in range(1, nx):
            s = plus_x(d)
            got(y_all_x.at[s, pl.ds(2 * pair, 2)], gxs_sem.at[d, k], gxr_sem.at[s, pair], {"row_1": s})
    core_own[1] = tdot(nb_rows, rows_of(y_all_x))
    ritz_core = send(core_own.at[1], core_par.at[1], cs_sem.at[4], cr_sem.at[4], {"col": other})

    for d in range(1, nx):
        s = plus_x(d)
        got(sq_all_x.at[s], qxs_sem.at[d], qxr_sem.at[s], {"row_1": s})
    sq_own[...] = jnp.sum(sq_all_x[...], axis=0)
    sq_core = send(sq_own, sq_par, cs_sem.at[3], cr_sem.at[3], {"col": other})
    metric_core.wait_recv()
    metric_ref[...] = core_own[0] + core_par[0]
    small_ref[7:8, :] = jnp.zeros((1, small_ref.shape[1]), jnp.float32)
    sq_core.wait_recv()
    for q in range(2):
        small_ref[6:7, q * LANES : (q + 1) * LANES] = sq_own[q : q + 1, :] + sq_par[q : q + 1, :]
    ritz_core.wait_recv()
    ritz_ref[...] = core_own[1] + core_par[1]

    for copy in copies:
        copy.wait_send()


def finish(window_total, small_in, ritz_in, metric_in, nb_ref, nd_ref, nc_ref, ritz_ref, metric_ref):
    ritz_ref[...] = ritz_in[...]
    metric_ref[...] = metric_in[...]
    nb_ref[...] = small_in[0:2, :]
    nd_ref[...] = small_in[2:4, :]
    nc_ref[...] = small_in[4:6, :] * lax.rsqrt(small_in[6:7, :] / window_total + 1e-06)


def on_device(hamiltonian_rows, current_block, correction_block, previous_block, ritz_values, mixing_coeffs):
    nz, nx = lax.axis_size("row_0"), lax.axis_size("row_1")
    pairs = nz // 2
    owners, _, out_rows, columns = hamiltonian_rows.shape
    block_width = current_block.shape[1]
    window_total = out_rows * owners * lax.axis_size("col")
    tiles = columns // LANES
    h_flat = hamiltonian_rows.reshape(owners, out_rows, tiles, LANES).transpose(0, 2, 1, 3)
    h_flat = h_flat.reshape(owners * tiles * out_rows, LANES)
    f32 = functools.partial(jax.ShapeDtypeStruct, dtype=jnp.float32)
    vmem = pl.BlockSpec(memory_space=pltpu.VMEM)
    hbm = pl.BlockSpec(memory_space=pltpu.HBM)
    square = (block_width, block_width)

    def buffer(*shape):
        return pltpu.VMEM(shape, jnp.float32)

    sems = pltpu.SemaphoreType.DMA
    sem_shapes = (
        [(6,)]
        + [(nx, pairs)] * 4
        + [(pairs,)] * 4
        + [(nz,)] * 6
        + [(nx, pairs)] * 2
        + [(nz,)] * 2
        + [(nx,)] * 2
        + [(nz,)] * 2
        + [(nx,)] * 2
        + [(5,)] * 2
    )
    chunk = (4, LANES)
    small, ritz, metric = pl.pallas_call(
        functools.partial(kernel, nz, nx),
        out_shape=(f32((8, block_width)), f32(square), f32(square)),
        in_specs=[hbm] * 6,
        out_specs=(vmem,) * 3,
        scratch_shapes=[
            buffer(1, block_width),
            buffer(*h_flat.shape),
            buffer(*square),
            buffer(*square),
            buffer(*square),
            buffer(*mixing_coeffs.shape),
            buffer(*square),
            buffer(*square),
            buffer(*square),
            buffer(nz, nx, *chunk),
            buffer(nz, nx, *chunk),
            buffer(nx, nz, *chunk),
            buffer(nx, nz, *chunk),
            buffer(pairs, 2, *chunk),
            buffer(pairs, 2, *chunk),
            buffer(pairs, 2, *chunk),
            buffer(pairs, 2, *chunk),
            buffer(nz, *chunk),
            buffer(nz, *chunk),
            buffer(nz, *chunk),
            buffer(nz, *chunk),
            buffer(*chunk),
            buffer(*chunk),
            buffer(nz, *chunk),
            buffer(nx, nz, *chunk),
            buffer(2, LANES),
            buffer(nz, 2, LANES),
            buffer(2, LANES),
            buffer(nx, 2, LANES),
            buffer(*chunk),
            buffer(nz, *chunk),
            buffer(nx, nz, *chunk),
            buffer(2, *square),
            buffer(2, *square),
            buffer(2, LANES),
            buffer(2, LANES),
        ]
        + [sems(shape) for shape in sem_shapes],
        compiler_params=pltpu.CompilerParams(
            collective_id=0, has_side_effects=True, vmem_limit_bytes=MAIN_VMEM
        ),
        name="lobpcg_step",
    )(
        *(
            pltpu.with_memory_space_constraint(a, pltpu.HBM)
            for a in (
                h_flat,
                current_block,
                correction_block,
                previous_block,
                mixing_coeffs,
                ritz_values.reshape(1, -1),
            )
        )
    )
    return pl.pallas_call(
        functools.partial(finish, window_total),
        out_shape=(f32((out_rows, block_width)),) * 3 + (f32(square),) * 2,
        in_specs=[vmem] * 3,
        out_specs=(vmem,) * 5,
        compiler_params=pltpu.CompilerParams(vmem_limit_bytes=END_VMEM),
        name="finish",
    )(small, ritz, metric)


def solution(mesh):
    finer = Mesh(
        mesh.devices.reshape(mesh.shape["chan"], NZ, NX, mesh.shape["col"]),
        ("chan", "row_0", "row_1", "col"),
    )
    in_specs = (
        P("chan", "col", None, ROW),
        P(CHAN_ROW_COL, None),
        P(CHAN_ROW_COL, None),
        P(CHAN_ROW_COL, None),
        P("chan"),
        P("chan", None),
    )
    out_specs = (
        P(CHAN_ROW_COL, None),
        P(CHAN_ROW_COL, None),
        P(CHAN_ROW_COL, None),
        P("chan", None),
        P("chan", None),
    )
    return jax.shard_map(on_device, mesh=finer, in_specs=in_specs, out_specs=out_specs, check_vma=False)
```

```python
import functools

import jax
import jax.numpy as jnp
from jax import lax
from jax.experimental import pallas as pl
from jax.experimental.pallas import tpu as pltpu
from jax.sharding import Mesh
from jax.sharding import PartitionSpec as P

NZ, NX = 16, 8
ROW = ("row_0", "row_1")
CHAN_ROW_COL = ("chan", "row_0", "row_1", "col")
MESH = pl.DeviceIdType.MESH
LANES = 128
GROUP = 4
MAIN_VMEM = 24 * 2**20
END_VMEM = 8 * 2**20
HIGHEST = lax.Precision.HIGHEST


def dot(left, right):
    return jnp.dot(left, right, preferred_element_type=jnp.float32, precision=HIGHEST)


def tdot(left, right):
    return lax.dot_general(
        left,
        right,
        (((0,), (0,)), ((), ())),
        preferred_element_type=jnp.float32,
        precision=HIGHEST,
    )


def kernel(
    nz,
    nx,
    h_hbm,
    x_hbm,
    w_hbm,
    p_hbm,
    c_hbm,
    rv_hbm,
    small_ref,
    ritz_ref,
    metric_ref,
    rv_ref,
    h_ref,
    c_ref,
    rows,
    h_rows,
    prod,
    part,
    in_x,
    mid,
    in_z,
    tile,
    all_z,
    gathered,
    nb_tile,
    nb_all_z,
    nb_t,
    sq_tile,
    sq_all_z,
    sq_sum,
    sq_all_x,
    core_own,
    core_par,
    sq_own,
    sq_par,
    in_sem,
    xs_sem,
    xr_sem,
    zs_sem,
    zr_sem,
    gzs_sem,
    gzr_sem,
    gxs_sem,
    gxr_sem,
    qzs_sem,
    qzr_sem,
    qxs_sem,
    qxr_sem,
    nzs_sem,
    nzr_sem,
    nxs_sem,
    nxr_sem,
    cs_sem,
    cr_sem,
):
    z = lax.axis_index("row_0")
    x = lax.axis_index("row_1")
    core = lax.axis_index("col")
    other = 1 - core
    owners = nz * nx
    groups = nz // GROUP
    own_group = z // GROUP
    half = rows.shape[1]

    def plus_z(d):
        return lax.rem(z + d, nz)

    def plus_x(d):
        return lax.rem(x + d, nx)

    def far_group(k):
        step = (k + 1) // 2
        return lax.rem(own_group + groups // 2 + step * (1 - 2 * lax.rem(k, 2)) + groups, groups)

    def member(group, m):
        return group * GROUP + lax.rem(lax.rem(z, GROUP) + m, GROUP)

    def remote(src, dst, send, recv, device):
        return pltpu.make_async_remote_copy(
            src_ref=src, dst_ref=dst, send_sem=send, recv_sem=recv, device_id=device, device_id_type=MESH
        )

    def loop(first, last, body):
        def step(i, carry):
            body(i)
            return carry

        lax.fori_loop(first, last, step, 0)

    def send_all_z(src, into, s_sem, r_sem):
        loop(1, nz, lambda d: remote(src, into.at[z], s_sem.at[d], r_sem.at[z], {"row_0": plus_z(d)}).start())

    def got_all_z(into, s_sem, r_sem):
        loop(1, nz, lambda d: remote(into.at[z], into.at[z], s_sem.at[d], r_sem.at[plus_z(d)], {"row_0": z}).wait_recv())

    def sent_all_z(src, s_sem, r_sem):
        loop(1, nz, lambda d: remote(src, src, s_sem.at[d], r_sem.at[z], {"row_0": z}).wait_send())

    def send_all_x(src, into, s_sem, r_sem):
        loop(1, nx, lambda d: remote(src, into.at[x], s_sem.at[d], r_sem.at[x], {"row_1": plus_x(d)}).start())

    def got_all_x(into, s_sem, r_sem):
        loop(1, nx, lambda d: remote(into.at[x], into.at[x], s_sem.at[d], r_sem.at[plus_x(d)], {"row_1": x}).wait_recv())

    def sent_all_x(src, s_sem, r_sem):
        loop(1, nx, lambda d: remote(src, src, s_sem.at[d], r_sem.at[x], {"row_1": x}).wait_send())

    def core_copy(src, dst, i):
        return remote(src, dst, cs_sem.at[i], cr_sem.at[i], {"col": other})

    loads = []
    for i, (src, dst) in enumerate(
        [
            (w_hbm, rows.at[0]),
            (c_hbm.at[pl.ds(half, half)], c_ref.at[0]),
            (p_hbm, rows.at[1]),
            (c_hbm.at[pl.ds(2 * half, half)], c_ref.at[1]),
            (x_hbm, rows.at[2]),
            (c_hbm.at[pl.ds(0, half)], c_ref.at[2]),
            (h_hbm, h_ref),
            (rv_hbm, rv_ref),
        ]
    ):
        loads.append(pltpu.make_async_copy(src, dst, in_sem.at[i]))
        loads[i].start()

    barrier = pltpu.get_barrier_semaphore()
    loop(1, nz, lambda d: pl.semaphore_signal(barrier, inc=1, device_id={"row_0": plus_z(d)}, device_id_type=MESH))
    loop(1, nx, lambda d: pl.semaphore_signal(barrier, inc=1, device_id={"row_1": plus_x(d)}, device_id_type=MESH))
    pl.semaphore_signal(barrier, inc=1, device_id={"col": other}, device_id_type=MESH)

    for load in loads[:6]:
        load.wait()

    rows[4] = jnp.zeros(rows.shape[1:], jnp.float32)

    def add_product(i):
        small_ref[2:4, :] = rows[4, 0:2, :]
        rows[4] += dot(rows[i], c_ref[i])

    loop(0, 3, add_product)
    small_ref[0:2, :] = rows[4, 0:2, :]
    for j in range(2):
        for q in range(2):
            nb_tile[j * 2 + q : j * 2 + q + 1, :] = rows[4, j : j + 1, q * LANES : (q + 1) * LANES]

    pl.semaphore_wait(barrier, nz + nx - 1)
    y_core = core_copy(rows.at[4], rows.at[5], 1)
    y_core.start()
    x_core = core_copy(rows.at[2], rows.at[3], 0)
    x_core.start()
    send_all_z(nb_tile, nb_all_z, nzs_sem, nzr_sem)

    loads[6].wait()
    loads[7].wait()
    tiles = half // LANES

    def order(n):
        i = n // nx
        owner_x = lax.rem(n, nx)
        which = core + i - 2 * core * i
        for j in range(2):
            to = pl.multiple_of(j * owners + owner_x * nz, nz)
            for t in range(tiles):
                h_rows[i, pl.ds(to, nz), t * LANES : (t + 1) * LANES] = h_ref[
                    pl.ds(owner_x * 8 + (which * tiles + t) * 2 + j, nz, stride=8 * nx), :
                ]

    loop(0, 2 * nx, order)

    def own_product(v):
        prod[v] = dot(h_rows[0], rows[4 - 2 * v])

    loop(0, 2, own_product)
    y_core.wait_recv()
    x_core.wait_recv()

    def other_product(v):
        value = prod[v] + dot(h_rows[1], rows[5 - 2 * v])
        for j in range(2):
            for q in range(2):
                block = value[j * owners : (j + 1) * owners, q * LANES : (q + 1) * LANES]
                part[v, :, :, j * 2 + q, :] = block.reshape(nx, nz, LANES)

        def send_group(k):
            group = far_group(k)
            members = pl.ds(group * GROUP, GROUP)
            loop(
                1,
                nx,
                lambda d: remote(
                    part.at[v, plus_x(d), members],
                    in_x.at[v, x, members],
                    xs_sem.at[v, group, d],
                    xr_sem.at[v, group, x],
                    {"row_1": plus_x(d)},
                ).start(),
            )

        loop(0, groups, send_group)

    loop(0, 2, other_product)

    def pass_group(n):
        v = n // groups
        k = lax.rem(n, groups)
        group = far_group(k)
        members = pl.ds(group * GROUP, GROUP)
        own = part.at[v, x, members]
        loop(
            1,
            nx,
            lambda d: remote(
                own, in_x.at[v, x, members], xs_sem.at[v, group, d], xr_sem.at[v, group, plus_x(d)], {"row_1": x}
            ).wait_recv(),
        )
        total = part[v, x, members]
        for d in range(1, nx):
            total = total + in_x[v, plus_x(d), members]
        mid[v, members] = total

        def send_member(m):
            to = member(group, m)
            remote(mid.at[v, to], in_z.at[v, z], zs_sem.at[v, to], zr_sem.at[v, z], {"row_0": to}).start()

        @pl.when(k < groups - 1)
        def _():
            send_member(0)

        loop(1, GROUP, send_member)

    loop(0, 2 * groups, pass_group)

    def sum_z(v):
        loop(
            1,
            nz,
            lambda d: remote(
                mid.at[v, z], in_z.at[v, z], zs_sem.at[v, z], zr_sem.at[v, plus_z(d)], {"row_0": z}
            ).wait_recv(),
        )
        total = mid[v, z]
        for d in range(1, nz):
            total = total + in_z[v, plus_z(d)]
        tile[v] = total

    sum_z(0)
    send_all_z(tile.at[0], all_z, gzs_sem, gzr_sem)
    all_z[z] = tile[0]

    got_all_z(nb_all_z, nzs_sem, nzr_sem)
    nb_all_z[z] = nb_tile[...]
    send_all_x(nb_all_z, gathered.at[0], nxs_sem, nxr_sem)
    gathered[0, x] = nb_all_z[...]

    sum_z(1)
    for q in range(2):
        squares = 0.0
        for j in range(2):
            columns = slice(q * LANES, (q + 1) * LANES)
            residual = tile[1, j * 2 + q : j * 2 + q + 1, :] - rows[2, j : j + 1, columns] * rv_ref[:, columns]
            small_ref[4 + j : 5 + j, columns] = residual
            squares = squares + residual * residual
        sq_tile[q : q + 1, :] = squares
    send_all_z(sq_tile, sq_all_z, qzs_sem, qzr_sem)
    sq_all_z[z] = sq_tile[...]

    def forward(n):
        k = groups - 1 - n
        group = far_group(k)
        members = pl.ds(group * GROUP, GROUP)

        def got_member(m):
            s = member(group, m)
            remote(all_z.at[s], all_z.at[s], gzs_sem.at[0], gzr_sem.at[s], {"row_0": z}).wait_recv()

        @pl.when(k < groups - 1)
        def _():
            got_member(0)

        loop(1, GROUP, got_member)
        loop(
            1,
            nx,
            lambda d: remote(
                all_z.at[members],
                gathered.at[1, x, members],
                gxs_sem.at[group, d],
                gxr_sem.at[group, x],
                {"row_1": plus_x(d)},
            ).start(),
        )

    loop(0, groups, forward)
    gathered[1, x] = all_z[...]

    def rows_of(u):
        columns = []
        for q in range(2):
            columns.append(
                jnp.concatenate([gathered[u, :, :, 2 * j + q, :].reshape(owners, LANES) for j in range(2)], axis=0)
            )
        return jnp.concatenate(columns, axis=1)

    got_all_x(gathered.at[0], nxs_sem, nxr_sem)
    nb_t[...] = rows_of(0).T

    def last_product(u):
        @pl.when(u == 1)
        def _():
            got_all_z(sq_all_z, qzs_sem, qzr_sem)
            sq_sum[...] = jnp.sum(sq_all_z[...], axis=0)
            send_all_x(sq_sum, sq_all_x, qxs_sem, qxr_sem)
            sq_all_x[x] = sq_sum[...]

            def got_group(group):
                members = pl.ds(group * GROUP, GROUP)
                loop(
                    1,
                    nx,
                    lambda d: remote(
                        all_z.at[members],
                        gathered.at[1, x, members],
                        gxs_sem.at[group, d],
                        gxr_sem.at[group, plus_x(d)],
                        {"row_1": x},
                    ).wait_recv(),
                )

            loop(0, groups, got_group)

        core_own[u] = dot(nb_t[...], rows_of(u))
        remote(core_own.at[u], core_par.at[u], cs_sem.at[2 + u], cr_sem.at[2 + u], {"col": other}).start()

    loop(0, 2, last_product)

    got_all_x(sq_all_x, qxs_sem, qxr_sem)
    sq_own[...] = jnp.sum(sq_all_x[...], axis=0)
    sq_core = core_copy(sq_own, sq_par, 4)
    sq_core.start()
    core_copy(core_own.at[0], core_par.at[0], 2).wait_recv()
    metric_ref[...] = core_own[0] + core_par[0]
    small_ref[7:8, :] = jnp.zeros((1, small_ref.shape[1]), jnp.float32)
    sq_core.wait_recv()
    for q in range(2):
        small_ref[6:7, q * LANES : (q + 1) * LANES] = sq_own[q : q + 1, :] + sq_par[q : q + 1, :]

    y_core.wait_send()
    x_core.wait_send()
    sent_all_z(nb_tile, nzs_sem, nzr_sem)
    sent_all_z(tile.at[0], gzs_sem, gzr_sem)
    sent_all_z(sq_tile, qzs_sem, qzr_sem)
    sent_all_x(nb_all_z, nxs_sem, nxr_sem)
    sent_all_x(sq_sum, qxs_sem, qxr_sem)

    def sent_sums(n):
        v = n // groups
        group = lax.rem(n, groups)
        members = pl.ds(group * GROUP, GROUP)
        own = part.at[v, x, members]
        loop(
            1,
            nx,
            lambda d: remote(own, own, xs_sem.at[v, group, d], xr_sem.at[v, group, x], {"row_1": x}).wait_send(),
        )

    loop(0, 2 * groups, sent_sums)

    def sent_mid(n):
        v = n // nz
        d = lax.rem(n, nz)

        @pl.when(d > 0)
        def _():
            to = plus_z(d)
            remote(mid.at[v, to], mid.at[v, to], zs_sem.at[v, to], zr_sem.at[v, z], {"row_0": z}).wait_send()

    loop(0, 2 * nz, sent_mid)

    def sent_group(group):
        members = all_z.at[pl.ds(group * GROUP, GROUP)]
        loop(
            1,
            nx,
            lambda d: remote(members, members, gxs_sem.at[group, d], gxr_sem.at[group, x], {"row_1": x}).wait_send(),
        )

    loop(0, groups, sent_group)
    core_copy(core_own.at[0], core_par.at[0], 2).wait_send()
    sq_core.wait_send()
    core_copy(core_own.at[1], core_par.at[1], 3).wait()
    ritz_ref[...] = core_own[1] + core_par[1]


def finish(window_total, small_in, ritz_in, metric_in, nb_ref, nd_ref, nc_ref, ritz_ref, metric_ref):
    ritz_ref[...] = ritz_in[...]
    metric_ref[...] = metric_in[...]
    nb_ref[...] = small_in[0:2, :]
    nd_ref[...] = small_in[2:4, :]
    nc_ref[...] = small_in[4:6, :] * lax.rsqrt(small_in[6:7, :] / window_total + 1e-06)


def on_device(hamiltonian_rows, current_block, correction_block, previous_block, ritz_values, mixing_coeffs):
    nz, nx = lax.axis_size("row_0"), lax.axis_size("row_1")
    groups = nz // GROUP
    owners, _, out_rows, columns = hamiltonian_rows.shape
    block_width = current_block.shape[1]
    window_total = out_rows * owners * lax.axis_size("col")
    tiles = columns // LANES
    h_flat = hamiltonian_rows.reshape(owners, out_rows, tiles, LANES).transpose(0, 2, 1, 3)
    h_flat = h_flat.reshape(owners * tiles * out_rows, LANES)
    f32 = functools.partial(jax.ShapeDtypeStruct, dtype=jnp.float32)
    vmem = pl.BlockSpec(memory_space=pltpu.VMEM)
    hbm = pl.BlockSpec(memory_space=pltpu.HBM)
    square = (block_width, block_width)

    def buffer(*shape):
        return pltpu.VMEM(shape, jnp.float32)

    sems = pltpu.SemaphoreType.DMA
    sem_shapes = (
        [(8,)]
        + [(2, groups, nx)] * 2
        + [(2, nz)] * 2
        + [(nz,)] * 2
        + [(groups, nx)] * 2
        + [(nz,)] * 2
        + [(nx,)] * 2
        + [(nz,)] * 2
        + [(nx,)] * 2
        + [(5,)] * 2
    )
    chunk = (4, LANES)
    small, ritz, metric = pl.pallas_call(
        functools.partial(kernel, nz, nx),
        out_shape=(f32((8, block_width)), f32(square), f32(square)),
        in_specs=[hbm] * 6,
        out_specs=(vmem,) * 3,
        scratch_shapes=[
            buffer(1, block_width),
            buffer(*h_flat.shape),
            buffer(3, *square),
            buffer(6, *square),
            buffer(2, 2 * owners, block_width),
            buffer(2, 2 * owners, block_width),
            buffer(2, nx, nz, *chunk),
            buffer(2, nx, nz, *chunk),
            buffer(2, nz, *chunk),
            buffer(2, nz, *chunk),
            buffer(2, *chunk),
            buffer(nz, *chunk),
            buffer(2, nx, nz, *chunk),
            buffer(*chunk),
            buffer(nz, *chunk),
            buffer(block_width, 2 * owners),
            buffer(2, LANES),
            buffer(nz, 2, LANES),
            buffer(2, LANES),
            buffer(nx, 2, LANES),
            buffer(2, *square),
            buffer(2, *square),
            buffer(2, LANES),
            buffer(2, LANES),
        ]
        + [sems(shape) for shape in sem_shapes],
        compiler_params=pltpu.CompilerParams(
            collective_id=0, has_side_effects=True, vmem_limit_bytes=MAIN_VMEM
        ),
        name="lobpcg_step",
    )(
        *(
            pltpu.with_memory_space_constraint(a, pltpu.HBM)
            for a in (
                h_flat,
                current_block,
                correction_block,
                previous_block,
                mixing_coeffs,
                ritz_values.reshape(1, -1),
            )
        )
    )
    return pl.pallas_call(
        functools.partial(finish, window_total),
        out_shape=(f32((out_rows, block_width)),) * 3 + (f32(square),) * 2,
        in_specs=[vmem] * 3,
        out_specs=(vmem,) * 5,
        compiler_params=pltpu.CompilerParams(vmem_limit_bytes=END_VMEM),
        name="finish",
    )(small, ritz, metric)


def solution(mesh):
    finer = Mesh(
        mesh.devices.reshape(mesh.shape["chan"], NZ, NX, mesh.shape["col"]),
        ("chan", "row_0", "row_1", "col"),
    )
    in_specs = (
        P("chan", "col", None, ROW),
        P(CHAN_ROW_COL, None),
        P(CHAN_ROW_COL, None),
        P(CHAN_ROW_COL, None),
        P("chan"),
        P("chan", None),
    )
    out_specs = (
        P(CHAN_ROW_COL, None),
        P(CHAN_ROW_COL, None),
        P(CHAN_ROW_COL, None),
        P("chan", None),
        P("chan", None),
    )
    return jax.shard_map(on_device, mesh=finer, in_specs=in_specs, out_specs=out_specs, check_vma=False)
```

```python
import functools

import jax
import jax.numpy as jnp
from jax import lax
from jax.experimental import pallas as pl
from jax.experimental.pallas import tpu as pltpu
from jax.sharding import Mesh
from jax.sharding import PartitionSpec as P

NZ, NX = 16, 8
ROW = ("row_0", "row_1")
CHAN_ROW_COL = ("chan", "row_0", "row_1", "col")
MESH = pl.DeviceIdType.MESH
LANES = 128
GROUP = 4
MAIN_VMEM = 24 * 2**20
END_VMEM = 8 * 2**20
HIGHEST = lax.Precision.HIGHEST


def dot(left, right):
    return jnp.dot(left, right, preferred_element_type=jnp.float32, precision=HIGHEST)


def tdot(left, right):
    return lax.dot_general(
        left,
        right,
        (((0,), (0,)), ((), ())),
        preferred_element_type=jnp.float32,
        precision=HIGHEST,
    )


def kernel(
    nz,
    nx,
    h_hbm,
    x_hbm,
    w_hbm,
    p_hbm,
    c_hbm,
    rv_hbm,
    small_ref,
    ritz_ref,
    metric_ref,
    rv_ref,
    h_ref,
    c_ref,
    rows,
    h_rows,
    prod,
    part,
    in_x,
    mid,
    in_z,
    tile,
    all_z,
    gathered,
    nb_tile,
    nb_all_z,
    nb_t,
    sq_tile,
    sq_all_z,
    sq_sum,
    sq_all_x,
    core_own,
    core_par,
    in_sem,
    xs_sem,
    xr_sem,
    zs_sem,
    zr_sem,
    gzs_sem,
    gzr_sem,
    gxs_sem,
    gxr_sem,
    qzs_sem,
    qzr_sem,
    qxs_sem,
    qxr_sem,
    nzs_sem,
    nzr_sem,
    nxs_sem,
    nxr_sem,
    cs_sem,
    cr_sem,
):
    z = lax.axis_index("row_0")
    x = lax.axis_index("row_1")
    core = lax.axis_index("col")
    other = 1 - core
    owners = nz * nx
    groups = nz // GROUP
    own_group = z // GROUP
    half = rows.shape[1]

    def plus_z(d):
        return lax.rem(z + d, nz)

    def plus_x(d):
        return lax.rem(x + d, nx)

    def far_group(k):
        step = (k + 1) // 2
        return lax.rem(own_group + groups // 2 + step * (1 - 2 * lax.rem(k, 2)) + groups, groups)

    def member(group, m):
        return group * GROUP + lax.rem(lax.rem(z, GROUP) + m, GROUP)

    def remote(src, dst, send, recv, device):
        return pltpu.make_async_remote_copy(
            src_ref=src, dst_ref=dst, send_sem=send, recv_sem=recv, device_id=device, device_id_type=MESH
        )

    def loop(first, last, body):
        def step(i, carry):
            body(i)
            return carry

        lax.fori_loop(first, last, step, 0)

    def far(i, n):
        return n // 2 + (i + 1) // 2 * (1 - 2 * lax.rem(i, 2))

    def each_z(body):
        loop(0, nz - 1, lambda i: body(far(i, nz)))

    def each_x(body):
        loop(0, nx - 1, lambda i: body(far(i, nx)))

    def send_all_z(src, into, s_sem, r_sem):
        each_z(lambda d: remote(src, into.at[z], s_sem.at[d], r_sem.at[z], {"row_0": plus_z(d)}).start())

    def got_all_z(into, s_sem, r_sem):
        each_z(lambda d: remote(into.at[z], into.at[z], s_sem.at[d], r_sem.at[plus_z(d)], {"row_0": z}).wait_recv())

    def sent_all_z(src, s_sem, r_sem):
        each_z(lambda d: remote(src, src, s_sem.at[d], r_sem.at[z], {"row_0": z}).wait_send())

    def send_all_x(src, into, s_sem, r_sem):
        each_x(lambda d: remote(src, into.at[x], s_sem.at[d], r_sem.at[x], {"row_1": plus_x(d)}).start())

    def got_all_x(into, s_sem, r_sem):
        each_x(lambda d: remote(into.at[x], into.at[x], s_sem.at[d], r_sem.at[plus_x(d)], {"row_1": x}).wait_recv())

    def sent_all_x(src, s_sem, r_sem):
        each_x(lambda d: remote(src, src, s_sem.at[d], r_sem.at[x], {"row_1": x}).wait_send())

    def core_copy(src, dst, i):
        return remote(src, dst, cs_sem.at[i], cr_sem.at[i], {"col": other})

    loads = []
    for i, (src, dst) in enumerate(
        [
            (w_hbm, rows.at[0]),
            (c_hbm.at[pl.ds(half, half)], c_ref.at[0]),
            (p_hbm, rows.at[1]),
            (c_hbm.at[pl.ds(2 * half, half)], c_ref.at[1]),
            (x_hbm, rows.at[2]),
            (c_hbm.at[pl.ds(0, half)], c_ref.at[2]),
            (h_hbm, h_ref),
            (rv_hbm, rv_ref),
        ]
    ):
        loads.append(pltpu.make_async_copy(src, dst, in_sem.at[i]))
        loads[i].start()

    barrier = pltpu.get_barrier_semaphore()
    def signal(device):
        pl.semaphore_signal(barrier, inc=1, device_id=device, device_id_type=MESH)

    def both_cores(body):
        loop(1, 2 * nx, lambda n: body(n // nx, lax.rem(n, nx)))

    def core_of(which):
        return core + which * (1 - 2 * core)

    each_z(lambda d: signal({"row_0": plus_z(d)}))
    both_cores(lambda which, d: signal({"row_1": plus_x(d), "col": core_of(which)}))

    for load in loads[:6]:
        load.wait()

    rows[4] = jnp.zeros(rows.shape[1:], jnp.float32)

    def add_product(i):
        small_ref[2:4, :] = rows[4, 0:2, :]
        rows[4] += dot(rows[i], c_ref[i])

    loop(0, 3, add_product)
    small_ref[0:2, :] = rows[4, 0:2, :]
    for j in range(2):
        for q in range(2):
            nb_tile[j * 2 + q : j * 2 + q + 1, :] = rows[4, j : j + 1, q * LANES : (q + 1) * LANES]

    pl.semaphore_wait(barrier, nz - 1 + 2 * nx - 1)
    y_core = core_copy(rows.at[4], rows.at[5], 1)
    y_core.start()
    x_core = core_copy(rows.at[2], rows.at[3], 0)
    x_core.start()
    send_all_z(nb_tile, nb_all_z, nzs_sem, nzr_sem)

    loads[6].wait()
    loads[7].wait()
    tiles = half // LANES

    def order(n):
        i = n // nx
        owner_x = lax.rem(n, nx)
        which = core + i - 2 * core * i
        for j in range(2):
            to = pl.multiple_of(j * owners + owner_x * nz, nz)
            for t in range(tiles):
                h_rows[i, pl.ds(to, nz), t * LANES : (t + 1) * LANES] = h_ref[
                    pl.ds(owner_x * 8 + (which * tiles + t) * 2 + j, nz, stride=8 * nx), :
                ]

    loop(0, 2 * nx, order)

    def own_product(v):
        prod[v] = dot(h_rows[0], rows[4 - 2 * v])

    loop(0, 2, own_product)
    y_core.wait_recv()
    x_core.wait_recv()

    def other_product(v):
        value = prod[v] + dot(h_rows[1], rows[5 - 2 * v])
        for j in range(2):
            for q in range(2):
                block = value[j * owners : (j + 1) * owners, q * LANES : (q + 1) * LANES]
                part[v, :, :, j * 2 + q, :] = block.reshape(nx, nz, LANES)

        each_x(
            lambda d: remote(
                part.at[v, plus_x(d)], in_x.at[v, x], xs_sem.at[v, d], xr_sem.at[v, x], {"row_1": plus_x(d)}
            ).start()
        )

    loop(0, 2, other_product)

    def sum_x(v):
        own = part.at[v, x]
        each_x(
            lambda d: remote(own, in_x.at[v, x], xs_sem.at[v, d], xr_sem.at[v, plus_x(d)], {"row_1": x}).wait_recv()
        )
        total = part[v, x]
        for d in range(1, nx):
            total = total + in_x[v, plus_x(d)]
        mid[v] = total
        each_z(
            lambda d: remote(
                mid.at[v, plus_z(d)], in_z.at[v, z], zs_sem.at[v, d], zr_sem.at[v, z], {"row_0": plus_z(d)}
            ).start()
        )

    def sum_z(v):
        each_z(
            lambda d: remote(
                mid.at[v, z], in_z.at[v, z], zs_sem.at[v, d], zr_sem.at[v, plus_z(d)], {"row_0": z}
            ).wait_recv()
        )
        total = mid[v, z]
        for d in range(1, nz):
            total = total + in_z[v, plus_z(d)]
        tile[v] = total

    sum_x(0)

    sum_z(0)
    send_all_z(tile.at[0], all_z, gzs_sem, gzr_sem)
    all_z[z] = tile[0]

    def forward(n):
        k = groups - 1 - n
        group = far_group(k)
        members = pl.ds(group * GROUP, GROUP)

        def got_member(m):
            s = member(group, m)
            remote(all_z.at[s], all_z.at[s], gzs_sem.at[0], gzr_sem.at[s], {"row_0": z}).wait_recv()

        @pl.when(k < groups - 1)
        def _():
            got_member(0)

        loop(1, GROUP, got_member)
        loop(
            1,
            nx,
            lambda d: remote(
                all_z.at[members],
                gathered.at[1, x, members],
                gxs_sem.at[group, d],
                gxr_sem.at[group, x],
                {"row_1": plus_x(d)},
            ).start(),
        )

    got_all_z(nb_all_z, nzs_sem, nzr_sem)
    nb_all_z[z] = nb_tile[...]
    send_all_x(nb_all_z, gathered.at[0], nxs_sem, nxr_sem)
    gathered[0, x] = nb_all_z[...]

    sum_x(1)
    forward(0)
    sum_z(1)
    for q in range(2):
        squares = 0.0
        for j in range(2):
            columns = slice(q * LANES, (q + 1) * LANES)
            residual = tile[1, j * 2 + q : j * 2 + q + 1, :] - rows[2, j : j + 1, columns] * rv_ref[:, columns]
            small_ref[4 + j : 5 + j, columns] = residual
            squares = squares + residual * residual
        sq_tile[q : q + 1, :] = squares
    send_all_z(sq_tile, sq_all_z, qzs_sem, qzr_sem)
    sq_all_z[z] = sq_tile[...]

    loop(1, groups, forward)
    gathered[1, x] = all_z[...]

    def rows_of(u):
        columns = []
        for q in range(2):
            columns.append(
                jnp.concatenate([gathered[u, :, :, 2 * j + q, :].reshape(owners, LANES) for j in range(2)], axis=0)
            )
        return jnp.concatenate(columns, axis=1)

    got_all_x(gathered.at[0], nxs_sem, nxr_sem)
    nb_t[...] = rows_of(0).T

    def last_product(u):
        @pl.when(u == 1)
        def _():
            def got_group(group):
                members = pl.ds(group * GROUP, GROUP)
                loop(
                    1,
                    nx,
                    lambda d: remote(
                        all_z.at[members],
                        gathered.at[1, x, members],
                        gxs_sem.at[group, d],
                        gxr_sem.at[group, plus_x(d)],
                        {"row_1": x},
                    ).wait_recv(),
                )

            loop(0, groups, got_group)

        core_own[u] = dot(nb_t[...], rows_of(u))
        remote(core_own.at[u], core_par.at[u], cs_sem.at[2 + u], cr_sem.at[2 + u], {"col": other}).start()

    loop(0, 2, last_product)

    got_all_z(sq_all_z, qzs_sem, qzr_sem)
    sq_sum[...] = jnp.sum(sq_all_z[...], axis=0)
    both_cores(
        lambda which, d: remote(
            sq_sum,
            sq_all_x.at[core, x],
            qxs_sem.at[which, d],
            qxr_sem.at[core, x],
            {"row_1": plus_x(d), "col": core_of(which)},
        ).start()
    )
    sq_all_x[core, x] = sq_sum[...]
    core_copy(core_own.at[0], core_par.at[0], 2).wait_recv()
    metric_ref[...] = core_own[0] + core_par[0]
    small_ref[7:8, :] = jnp.zeros((1, small_ref.shape[1]), jnp.float32)

    y_core.wait_send()
    x_core.wait_send()
    sent_all_z(nb_tile, nzs_sem, nzr_sem)
    sent_all_z(tile.at[0], gzs_sem, gzr_sem)
    sent_all_z(sq_tile, qzs_sem, qzr_sem)
    sent_all_x(nb_all_z, nxs_sem, nxr_sem)

    def sent_sums(v):
        each_x(
            lambda d: remote(part.at[v, x], part.at[v, x], xs_sem.at[v, d], xr_sem.at[v, x], {"row_1": x}).wait_send()
        )
        each_z(
            lambda d: remote(mid.at[v, z], mid.at[v, z], zs_sem.at[v, d], zr_sem.at[v, z], {"row_0": z}).wait_send()
        )

    loop(0, 2, sent_sums)

    def sent_group(group):
        members = all_z.at[pl.ds(group * GROUP, GROUP)]
        loop(
            1,
            nx,
            lambda d: remote(members, members, gxs_sem.at[group, d], gxr_sem.at[group, x], {"row_1": x}).wait_send(),
        )

    loop(0, groups, sent_group)
    core_copy(core_own.at[0], core_par.at[0], 2).wait_send()
    core_copy(core_own.at[1], core_par.at[1], 3).wait()
    ritz_ref[...] = core_own[1] + core_par[1]
    both_cores(
        lambda which, d: remote(
            sq_sum,
            sq_all_x.at[core, x],
            qxs_sem.at[which, d],
            qxr_sem.at[core_of(which), plus_x(d)],
            {"row_1": x, "col": other},
        ).wait()
    )
    squares = jnp.sum(jnp.sum(sq_all_x[...], axis=0), axis=0)
    for q in range(2):
        small_ref[6:7, q * LANES : (q + 1) * LANES] = squares[q : q + 1, :]


def finish(window_total, small_in, ritz_in, metric_in, nb_ref, nd_ref, nc_ref, ritz_ref, metric_ref):
    ritz_ref[...] = ritz_in[...]
    metric_ref[...] = metric_in[...]
    nb_ref[...] = small_in[0:2, :]
    nd_ref[...] = small_in[2:4, :]
    nc_ref[...] = small_in[4:6, :] * lax.rsqrt(small_in[6:7, :] / window_total + 1e-06)


def on_device(hamiltonian_rows, current_block, correction_block, previous_block, ritz_values, mixing_coeffs):
    nz, nx = lax.axis_size("row_0"), lax.axis_size("row_1")
    groups = nz // GROUP
    owners, _, out_rows, columns = hamiltonian_rows.shape
    block_width = current_block.shape[1]
    window_total = out_rows * owners * lax.axis_size("col")
    tiles = columns // LANES
    h_flat = hamiltonian_rows.reshape(owners, out_rows, tiles, LANES).transpose(0, 2, 1, 3)
    h_flat = h_flat.reshape(owners * tiles * out_rows, LANES)
    f32 = functools.partial(jax.ShapeDtypeStruct, dtype=jnp.float32)
    vmem = pl.BlockSpec(memory_space=pltpu.VMEM)
    hbm = pl.BlockSpec(memory_space=pltpu.HBM)
    square = (block_width, block_width)

    def buffer(*shape):
        return pltpu.VMEM(shape, jnp.float32)

    sems = pltpu.SemaphoreType.DMA
    sem_shapes = (
        [(8,)]
        + [(2, nx)] * 2
        + [(2, nz)] * 2
        + [(nz,)] * 2
        + [(groups, nx)] * 2
        + [(nz,)] * 2
        + [(2, nx)] * 2
        + [(nz,)] * 2
        + [(nx,)] * 2
        + [(4,)] * 2
    )
    chunk = (4, LANES)
    small, ritz, metric = pl.pallas_call(
        functools.partial(kernel, nz, nx),
        out_shape=(f32((8, block_width)), f32(square), f32(square)),
        in_specs=[hbm] * 6,
        out_specs=(vmem,) * 3,
        scratch_shapes=[
            buffer(1, block_width),
            buffer(*h_flat.shape),
            buffer(3, *square),
            buffer(6, *square),
            buffer(2, 2 * owners, block_width),
            buffer(2, 2 * owners, block_width),
            buffer(2, nx, nz, *chunk),
            buffer(2, nx, nz, *chunk),
            buffer(2, nz, *chunk),
            buffer(2, nz, *chunk),
            buffer(2, *chunk),
            buffer(nz, *chunk),
            buffer(2, nx, nz, *chunk),
            buffer(*chunk),
            buffer(nz, *chunk),
            buffer(block_width, 2 * owners),
            buffer(2, LANES),
            buffer(nz, 2, LANES),
            buffer(2, LANES),
            buffer(2, nx, 2, LANES),
            buffer(2, *square),
            buffer(2, *square),
        ]
        + [sems(shape) for shape in sem_shapes],
        compiler_params=pltpu.CompilerParams(
            collective_id=0, has_side_effects=True, vmem_limit_bytes=MAIN_VMEM
        ),
        name="lobpcg_step",
    )(
        *(
            pltpu.with_memory_space_constraint(a, pltpu.HBM)
            for a in (
                h_flat,
                current_block,
                correction_block,
                previous_block,
                mixing_coeffs,
                ritz_values.reshape(1, -1),
            )
        )
    )
    return pl.pallas_call(
        functools.partial(finish, window_total),
        out_shape=(f32((out_rows, block_width)),) * 3 + (f32(square),) * 2,
        in_specs=[vmem] * 3,
        out_specs=(vmem,) * 5,
        compiler_params=pltpu.CompilerParams(vmem_limit_bytes=END_VMEM),
        name="finish",
    )(small, ritz, metric)


def solution(mesh):
    finer = Mesh(
        mesh.devices.reshape(mesh.shape["chan"], NZ, NX, mesh.shape["col"]),
        ("chan", "row_0", "row_1", "col"),
    )
    in_specs = (
        P("chan", "col", None, ROW),
        P(CHAN_ROW_COL, None),
        P(CHAN_ROW_COL, None),
        P(CHAN_ROW_COL, None),
        P("chan"),
        P("chan", None),
    )
    out_specs = (
        P(CHAN_ROW_COL, None),
        P(CHAN_ROW_COL, None),
        P(CHAN_ROW_COL, None),
        P("chan", None),
        P("chan", None),
    )
    return jax.shard_map(on_device, mesh=finer, in_specs=in_specs, out_specs=out_specs, check_vma=False)
```

```python
import functools

import jax
import jax.numpy as jnp
from jax import lax
from jax.experimental import pallas as pl
from jax.experimental.pallas import tpu as pltpu
from jax.sharding import Mesh
from jax.sharding import PartitionSpec as P

NZ, NX = 16, 8
ROW = ("row_0", "row_1")
CHAN_ROW_COL = ("chan", "row_0", "row_1", "col")
MESH = pl.DeviceIdType.MESH
LANES = 128
GROUP = 4
MAIN_VMEM = 24 * 2**20
END_VMEM = 8 * 2**20
HIGHEST = lax.Precision.HIGHEST


def dot(left, right):
    return jnp.dot(left, right, preferred_element_type=jnp.float32, precision=HIGHEST)


def tdot(left, right):
    return lax.dot_general(
        left,
        right,
        (((0,), (0,)), ((), ())),
        preferred_element_type=jnp.float32,
        precision=HIGHEST,
    )


def kernel(
    nz,
    nx,
    h_hbm,
    x_hbm,
    w_hbm,
    p_hbm,
    c_hbm,
    rv_hbm,
    small_ref,
    ritz_ref,
    metric_ref,
    rv_ref,
    h_ref,
    c_ref,
    rows,
    h_rows,
    prod,
    y_part,
    y_in,
    y_mid,
    y_mid_in,
    x_part,
    x_in,
    x_mid,
    x_mid_in,
    tile,
    all_z,
    gathered,
    nb_tile,
    nb_all_z,
    nb_t,
    sq_tile,
    sq_all_z,
    sq_sum,
    sq_all_x,
    core_own,
    core_par,
    in_sem,
    yxs_sem,
    yxr_sem,
    yzs_sem,
    yzr_sem,
    xzs_sem,
    xzr_sem,
    xxs_sem,
    xxr_sem,
    gzs_sem,
    gzr_sem,
    gxs_sem,
    gxr_sem,
    qzs_sem,
    qzr_sem,
    qxs_sem,
    qxr_sem,
    nzs_sem,
    nzr_sem,
    nxs_sem,
    nxr_sem,
    cs_sem,
    cr_sem,
):
    z = lax.axis_index("row_0")
    x = lax.axis_index("row_1")
    core = lax.axis_index("col")
    other = 1 - core
    owners = nz * nx
    groups = nz // GROUP
    own_group = z // GROUP
    half = rows.shape[1]

    def plus_z(d):
        return lax.rem(z + d, nz)

    def plus_x(d):
        return lax.rem(x + d, nx)

    def far_group(k):
        step = (k + 1) // 2
        return lax.rem(own_group + groups // 2 + step * (1 - 2 * lax.rem(k, 2)) + groups, groups)

    def member(group, m):
        return group * GROUP + lax.rem(lax.rem(z, GROUP) + m, GROUP)

    def remote(src, dst, send, recv, device):
        return pltpu.make_async_remote_copy(
            src_ref=src, dst_ref=dst, send_sem=send, recv_sem=recv, device_id=device, device_id_type=MESH
        )

    def loop(first, last, body):
        def step(i, carry):
            body(i)
            return carry

        lax.fori_loop(first, last, step, 0)

    def far(i, n):
        return n // 2 + (i + 1) // 2 * (1 - 2 * lax.rem(i, 2))

    def each_z(body):
        loop(0, nz - 1, lambda i: body(far(i, nz)))

    def each_x(body):
        loop(0, nx - 1, lambda i: body(far(i, nx)))

    def send_all_z(src, into, s_sem, r_sem):
        each_z(lambda d: remote(src, into.at[z], s_sem.at[d], r_sem.at[z], {"row_0": plus_z(d)}).start())

    def got_all_z(into, s_sem, r_sem):
        each_z(lambda d: remote(into.at[z], into.at[z], s_sem.at[d], r_sem.at[plus_z(d)], {"row_0": z}).wait_recv())

    def sent_all_z(src, s_sem, r_sem):
        each_z(lambda d: remote(src, src, s_sem.at[d], r_sem.at[z], {"row_0": z}).wait_send())

    def send_all_x(src, into, s_sem, r_sem):
        each_x(lambda d: remote(src, into.at[x], s_sem.at[d], r_sem.at[x], {"row_1": plus_x(d)}).start())

    def got_all_x(into, s_sem, r_sem):
        each_x(lambda d: remote(into.at[x], into.at[x], s_sem.at[d], r_sem.at[plus_x(d)], {"row_1": x}).wait_recv())

    def sent_all_x(src, s_sem, r_sem):
        each_x(lambda d: remote(src, src, s_sem.at[d], r_sem.at[x], {"row_1": x}).wait_send())

    def scatter_z(parts, into, s_sem, r_sem):
        each_z(
            lambda d: remote(
                parts.at[plus_z(d)], into.at[z], s_sem.at[d], r_sem.at[z], {"row_0": plus_z(d)}
            ).start()
        )

    def scatter_x(parts, into, s_sem, r_sem):
        each_x(
            lambda d: remote(
                parts.at[plus_x(d)], into.at[x], s_sem.at[d], r_sem.at[x], {"row_1": plus_x(d)}
            ).start()
        )

    def total_z(own, into):
        for d in range(1, nz):
            own = own + into[plus_z(d)]
        return own

    def total_x(own, into):
        for d in range(1, nx):
            own = own + into[plus_x(d)]
        return own

    def core_copy(src, dst, i):
        return remote(src, dst, cs_sem.at[i], cr_sem.at[i], {"col": other})

    loads = []
    for i, (src, dst) in enumerate(
        [
            (w_hbm, rows.at[0]),
            (c_hbm.at[pl.ds(half, half)], c_ref.at[0]),
            (p_hbm, rows.at[1]),
            (c_hbm.at[pl.ds(2 * half, half)], c_ref.at[1]),
            (x_hbm, rows.at[2]),
            (c_hbm.at[pl.ds(0, half)], c_ref.at[2]),
            (h_hbm, h_ref),
            (rv_hbm, rv_ref),
        ]
    ):
        loads.append(pltpu.make_async_copy(src, dst, in_sem.at[i]))
        loads[i].start()

    barrier = pltpu.get_barrier_semaphore()
    def signal(device):
        pl.semaphore_signal(barrier, inc=1, device_id=device, device_id_type=MESH)

    def both_cores(body):
        loop(1, 2 * nx, lambda n: body(n // nx, lax.rem(n, nx)))

    def core_of(which):
        return core + which * (1 - 2 * core)

    each_z(lambda d: signal({"row_0": plus_z(d)}))
    both_cores(lambda which, d: signal({"row_1": plus_x(d), "col": core_of(which)}))

    for load in loads[:6]:
        load.wait()

    rows[4] = jnp.zeros(rows.shape[1:], jnp.float32)

    def add_product(i):
        small_ref[2:4, :] = rows[4, 0:2, :]
        rows[4] += dot(rows[i], c_ref[i])

    loop(0, 3, add_product)
    small_ref[0:2, :] = rows[4, 0:2, :]
    for j in range(2):
        for q in range(2):
            nb_tile[j * 2 + q : j * 2 + q + 1, :] = rows[4, j : j + 1, q * LANES : (q + 1) * LANES]

    loads[6].wait()
    loads[7].wait()
    tiles = half // LANES

    def order(n):
        i = n // nx
        owner_x = lax.rem(n, nx)
        which = core + i - 2 * core * i
        for j in range(2):
            to = pl.multiple_of(j * owners + owner_x * nz, nz)
            for t in range(tiles):
                h_rows[i, pl.ds(to, nz), t * LANES : (t + 1) * LANES] = h_ref[
                    pl.ds(owner_x * 8 + (which * tiles + t) * 2 + j, nz, stride=8 * nx), :
                ]

    loop(0, 2 * nx, order)

    def own_product(v):
        prod[v] = dot(h_rows[0], rows[4 - 2 * v])

    loop(0, 2, own_product)
    pl.semaphore_wait(barrier, nz - 1 + 2 * nx - 1)
    y_core = core_copy(rows.at[4], rows.at[5], 1)
    y_core.start()
    x_core = core_copy(rows.at[2], rows.at[3], 0)
    x_core.start()
    send_all_z(nb_tile, nb_all_z, nzs_sem, nzr_sem)

    def other_product(v):
        @pl.when(v == 0)
        def _():
            y_core.wait_recv()

        @pl.when(v == 1)
        def _():
            x_core.wait_recv()

        prod[v] += dot(h_rows[1], rows[5 - 2 * v])

        def blocks():
            for j in range(2):
                for q in range(2):
                    block = prod[v, j * owners : (j + 1) * owners, q * LANES : (q + 1) * LANES]
                    yield j * 2 + q, block.reshape(nx, nz, LANES)

        @pl.when(v == 0)
        def _():
            for row, block in blocks():
                y_part[:, :, row, :] = block
            scatter_x(y_part, y_in, yxs_sem, yxr_sem)

        @pl.when(v == 1)
        def _():
            for row, block in blocks():
                for owner_x in range(nx):
                    x_part[:, owner_x, row, :] = block[owner_x]
            scatter_z(x_part, x_in, xzs_sem, xzr_sem)

    loop(0, 2, other_product)

    got_all_x(y_in, yxs_sem, yxr_sem)
    y_mid[...] = total_x(y_part[x], y_in)
    scatter_z(y_mid, y_mid_in, yzs_sem, yzr_sem)

    got_all_z(nb_all_z, nzs_sem, nzr_sem)
    nb_all_z[z] = nb_tile[...]
    send_all_x(nb_all_z, gathered.at[0], nxs_sem, nxr_sem)
    gathered[0, x] = nb_all_z[...]

    got_all_z(x_in, xzs_sem, xzr_sem)
    x_mid[...] = total_z(x_part[z], x_in)
    scatter_x(x_mid, x_mid_in, xxs_sem, xxr_sem)

    got_all_z(y_mid_in, yzs_sem, yzr_sem)
    tile[0] = total_z(y_mid[z], y_mid_in)
    send_all_z(tile.at[0], all_z, gzs_sem, gzr_sem)
    all_z[z] = tile[0]

    got_all_x(x_mid_in, xxs_sem, xxr_sem)
    tile[1] = total_x(x_mid[x], x_mid_in)
    for q in range(2):
        squares = 0.0
        for j in range(2):
            columns = slice(q * LANES, (q + 1) * LANES)
            residual = tile[1, j * 2 + q : j * 2 + q + 1, :] - rows[2, j : j + 1, columns] * rv_ref[:, columns]
            small_ref[4 + j : 5 + j, columns] = residual
            squares = squares + residual * residual
        sq_tile[q : q + 1, :] = squares
    send_all_z(sq_tile, sq_all_z, qzs_sem, qzr_sem)
    sq_all_z[z] = sq_tile[...]

    def forward(n):
        k = groups - 1 - n
        group = far_group(k)
        members = pl.ds(group * GROUP, GROUP)

        def got_member(m):
            s = member(group, m)
            remote(all_z.at[s], all_z.at[s], gzs_sem.at[0], gzr_sem.at[s], {"row_0": z}).wait_recv()

        @pl.when(k < groups - 1)
        def _():
            got_member(0)

        loop(1, GROUP, got_member)
        loop(
            1,
            nx,
            lambda d: remote(
                all_z.at[members],
                gathered.at[1, x, members],
                gxs_sem.at[group, d],
                gxr_sem.at[group, x],
                {"row_1": plus_x(d)},
            ).start(),
        )

    loop(0, groups, forward)
    gathered[1, x] = all_z[...]

    def rows_of(u):
        columns = []
        for q in range(2):
            columns.append(
                jnp.concatenate([gathered[u, :, :, 2 * j + q, :].reshape(owners, LANES) for j in range(2)], axis=0)
            )
        return jnp.concatenate(columns, axis=1)

    got_all_x(gathered.at[0], nxs_sem, nxr_sem)
    nb_t[...] = rows_of(0).T

    def last_product(u):
        @pl.when(u == 1)
        def _():
            got_all_z(sq_all_z, qzs_sem, qzr_sem)
            sq_sum[...] = jnp.sum(sq_all_z[...], axis=0)
            both_cores(
                lambda which, d: remote(
                    sq_sum,
                    sq_all_x.at[core, x],
                    qxs_sem.at[which, d],
                    qxr_sem.at[core, x],
                    {"row_1": plus_x(d), "col": core_of(which)},
                ).start()
            )
            sq_all_x[core, x] = sq_sum[...]

            def got_group(group):
                members = pl.ds(group * GROUP, GROUP)
                each_x(
                    lambda d: remote(
                        all_z.at[members],
                        gathered.at[1, x, members],
                        gxs_sem.at[group, d],
                        gxr_sem.at[group, plus_x(d)],
                        {"row_1": x},
                    ).wait_recv()
                )

            loop(0, groups, got_group)

        core_own[u] = dot(nb_t[...], rows_of(u))
        remote(core_own.at[u], core_par.at[u], cs_sem.at[2 + u], cr_sem.at[2 + u], {"col": other}).start()

        @pl.when(u == 0)
        def _():
            y_core.wait_send()
            x_core.wait_send()
            sent_all_z(nb_tile, nzs_sem, nzr_sem)
            sent_all_x(y_part.at[x], yxs_sem, yxr_sem)
            sent_all_z(y_mid.at[z], yzs_sem, yzr_sem)
            sent_all_z(x_part.at[z], xzs_sem, xzr_sem)
            sent_all_x(x_mid.at[x], xxs_sem, xxr_sem)
            sent_all_x(nb_all_z, nxs_sem, nxr_sem)
            sent_all_z(tile.at[0], gzs_sem, gzr_sem)

        @pl.when(u == 1)
        def _():
            core_copy(core_own.at[0], core_par.at[0], 2).wait()
            metric_ref[...] = core_own[0] + core_par[0]
            sent_all_z(sq_tile, qzs_sem, qzr_sem)

            def sent_group(group):
                members = all_z.at[pl.ds(group * GROUP, GROUP)]
                each_x(
                    lambda d: remote(
                        members, members, gxs_sem.at[group, d], gxr_sem.at[group, x], {"row_1": x}
                    ).wait_send()
                )

            loop(0, groups, sent_group)

    small_ref[7:8, :] = jnp.zeros((1, small_ref.shape[1]), jnp.float32)
    loop(0, 2, last_product)
    core_copy(core_own.at[1], core_par.at[1], 3).wait()
    ritz_ref[...] = core_own[1] + core_par[1]
    both_cores(
        lambda which, d: remote(
            sq_sum,
            sq_all_x.at[core, x],
            qxs_sem.at[which, d],
            qxr_sem.at[core_of(which), plus_x(d)],
            {"row_1": x, "col": other},
        ).wait()
    )
    squares = jnp.sum(jnp.sum(sq_all_x[...], axis=0), axis=0)
    for q in range(2):
        small_ref[6:7, q * LANES : (q + 1) * LANES] = squares[q : q + 1, :]


def finish(window_total, small_in, ritz_in, metric_in, nb_ref, nd_ref, nc_ref, ritz_ref, metric_ref):
    ritz_ref[...] = ritz_in[...]
    metric_ref[...] = metric_in[...]
    nb_ref[...] = small_in[0:2, :]
    nd_ref[...] = small_in[2:4, :]
    nc_ref[...] = small_in[4:6, :] * lax.rsqrt(small_in[6:7, :] / window_total + 1e-06)


def on_device(hamiltonian_rows, current_block, correction_block, previous_block, ritz_values, mixing_coeffs):
    nz, nx = lax.axis_size("row_0"), lax.axis_size("row_1")
    groups = nz // GROUP
    owners, _, out_rows, columns = hamiltonian_rows.shape
    block_width = current_block.shape[1]
    window_total = out_rows * owners * lax.axis_size("col")
    tiles = columns // LANES
    h_flat = hamiltonian_rows.reshape(owners, out_rows, tiles, LANES).transpose(0, 2, 1, 3)
    h_flat = h_flat.reshape(owners * tiles * out_rows, LANES)
    f32 = functools.partial(jax.ShapeDtypeStruct, dtype=jnp.float32)
    vmem = pl.BlockSpec(memory_space=pltpu.VMEM)
    hbm = pl.BlockSpec(memory_space=pltpu.HBM)
    square = (block_width, block_width)

    def buffer(*shape):
        return pltpu.VMEM(shape, jnp.float32)

    sems = pltpu.SemaphoreType.DMA
    sem_shapes = (
        [(8,)]
        + [(nx,)] * 2
        + [(nz,)] * 4
        + [(nx,)] * 2
        + [(nz,)] * 2
        + [(groups, nx)] * 2
        + [(nz,)] * 2
        + [(2, nx)] * 2
        + [(nz,)] * 2
        + [(nx,)] * 2
        + [(4,)] * 2
    )
    chunk = (4, LANES)
    small, ritz, metric = pl.pallas_call(
        functools.partial(kernel, nz, nx),
        out_shape=(f32((8, block_width)), f32(square), f32(square)),
        in_specs=[hbm] * 6,
        out_specs=(vmem,) * 3,
        scratch_shapes=[
            buffer(1, block_width),
            buffer(*h_flat.shape),
            buffer(3, *square),
            buffer(6, *square),
            buffer(2, 2 * owners, block_width),
            buffer(2, 2 * owners, block_width),
            buffer(nx, nz, *chunk),
            buffer(nx, nz, *chunk),
            buffer(nz, *chunk),
            buffer(nz, *chunk),
            buffer(nz, nx, *chunk),
            buffer(nz, nx, *chunk),
            buffer(nx, *chunk),
            buffer(nx, *chunk),
            buffer(2, *chunk),
            buffer(nz, *chunk),
            buffer(2, nx, nz, *chunk),
            buffer(*chunk),
            buffer(nz, *chunk),
            buffer(block_width, 2 * owners),
            buffer(2, LANES),
            buffer(nz, 2, LANES),
            buffer(2, LANES),
            buffer(2, nx, 2, LANES),
            buffer(2, *square),
            buffer(2, *square),
        ]
        + [sems(shape) for shape in sem_shapes],
        compiler_params=pltpu.CompilerParams(
            collective_id=0, has_side_effects=True, vmem_limit_bytes=MAIN_VMEM
        ),
        name="lobpcg_step",
    )(
        *(
            pltpu.with_memory_space_constraint(a, pltpu.HBM)
            for a in (
                h_flat,
                current_block,
                correction_block,
                previous_block,
                mixing_coeffs,
                ritz_values.reshape(1, -1),
            )
        )
    )
    return pl.pallas_call(
        functools.partial(finish, window_total),
        out_shape=(f32((out_rows, block_width)),) * 3 + (f32(square),) * 2,
        in_specs=[vmem] * 3,
        out_specs=(vmem,) * 5,
        compiler_params=pltpu.CompilerParams(vmem_limit_bytes=END_VMEM),
        name="finish",
    )(small, ritz, metric)


def solution(mesh):
    finer = Mesh(
        mesh.devices.reshape(mesh.shape["chan"], NZ, NX, mesh.shape["col"]),
        ("chan", "row_0", "row_1", "col"),
    )
    in_specs = (
        P("chan", "col", None, ROW),
        P(CHAN_ROW_COL, None),
        P(CHAN_ROW_COL, None),
        P(CHAN_ROW_COL, None),
        P("chan"),
        P("chan", None),
    )
    out_specs = (
        P(CHAN_ROW_COL, None),
        P(CHAN_ROW_COL, None),
        P(CHAN_ROW_COL, None),
        P("chan", None),
        P("chan", None),
    )
    return jax.shard_map(on_device, mesh=finer, in_specs=in_specs, out_specs=out_specs, check_vma=False)
```

```python
import functools

import jax
import jax.numpy as jnp
from jax import lax
from jax.experimental import pallas as pl
from jax.experimental.pallas import tpu as pltpu
from jax.sharding import Mesh
from jax.sharding import PartitionSpec as P

NZ, NX = 16, 8
ROW = ("row_0", "row_1")
CHAN_ROW_COL = ("chan", "row_0", "row_1", "col")
MESH = pl.DeviceIdType.MESH
LANES = 128
GROUP = 4
MAIN_VMEM = 24 * 2**20
END_VMEM = 8 * 2**20
HIGHEST = lax.Precision.HIGHEST


def dot(left, right):
    return jnp.dot(left, right, preferred_element_type=jnp.float32, precision=HIGHEST)


def tdot(left, right):
    return lax.dot_general(
        left,
        right,
        (((0,), (0,)), ((), ())),
        preferred_element_type=jnp.float32,
        precision=HIGHEST,
    )


def kernel(
    nz,
    nx,
    h_hbm,
    x_hbm,
    w_hbm,
    p_hbm,
    c_hbm,
    rv_hbm,
    small_ref,
    ritz_ref,
    metric_ref,
    rv_ref,
    h_ref,
    c_ref,
    rows,
    h_rows,
    prod,
    part,
    part_in,
    hop_in,
    hop,
    mid,
    mid_in,
    tile,
    all_z,
    gathered,
    nb_tile,
    nb_all_z,
    nb_t,
    sq_tile,
    sq_all_z,
    sq_sum,
    sq_all_x,
    core_own,
    core_par,
    in_sem,
    ps_sem,
    pr_sem,
    fs_sem,
    fr_sem,
    hs_sem,
    hr_sem,
    zs_sem,
    zr_sem,
    gzs_sem,
    gzr_sem,
    gxs_sem,
    gxr_sem,
    qzs_sem,
    qzr_sem,
    qxs_sem,
    qxr_sem,
    nzs_sem,
    nzr_sem,
    nxs_sem,
    nxr_sem,
    cs_sem,
    cr_sem,
):
    z = lax.axis_index("row_0")
    x = lax.axis_index("row_1")
    core = lax.axis_index("col")
    other = 1 - core
    owners = nz * nx
    groups = nz // GROUP
    own_group = z // GROUP
    half = rows.shape[1]

    def plus_z(d):
        return lax.rem(z + d, nz)

    def plus_x(d):
        return lax.rem(x + d + nx, nx)

    def far_group(k):
        step = (k + 1) // 2
        return lax.rem(own_group + groups // 2 + step * (1 - 2 * lax.rem(k, 2)) + groups, groups)

    def member(group, m):
        return group * GROUP + lax.rem(lax.rem(z, GROUP) + m, GROUP)

    def remote(src, dst, send, recv, device):
        return pltpu.make_async_remote_copy(
            src_ref=src, dst_ref=dst, send_sem=send, recv_sem=recv, device_id=device, device_id_type=MESH
        )

    def loop(first, last, body):
        def step(i, carry):
            body(i)
            return carry

        lax.fori_loop(first, last, step, 0)

    def far(i, n):
        return n // 2 + (i + 1) // 2 * (1 - 2 * lax.rem(i, 2))

    def each_z(body):
        loop(0, nz - 1, lambda i: body(far(i, nz)))

    def each_x(body):
        loop(0, nx - 1, lambda i: body(far(i, nx)))

    def send_all_z(src, into, s_sem, r_sem):
        each_z(lambda d: remote(src, into.at[z], s_sem.at[d], r_sem.at[z], {"row_0": plus_z(d)}).start())

    def got_all_z(into, s_sem, r_sem):
        each_z(lambda d: remote(into.at[z], into.at[z], s_sem.at[d], r_sem.at[plus_z(d)], {"row_0": z}).wait_recv())

    def sent_all_z(src, s_sem, r_sem):
        each_z(lambda d: remote(src, src, s_sem.at[d], r_sem.at[z], {"row_0": z}).wait_send())

    def send_all_x(src, into, s_sem, r_sem):
        each_x(lambda d: remote(src, into.at[x], s_sem.at[d], r_sem.at[x], {"row_1": plus_x(d)}).start())

    def got_all_x(into, s_sem, r_sem):
        each_x(lambda d: remote(into.at[x], into.at[x], s_sem.at[d], r_sem.at[plus_x(d)], {"row_1": x}).wait_recv())

    def sent_all_x(src, s_sem, r_sem):
        each_x(lambda d: remote(src, src, s_sem.at[d], r_sem.at[x], {"row_1": x}).wait_send())

    opposite = nx // 2
    whole = [d for d in range(1 - opposite, opposite) if abs(d) not in (0, opposite - 1)]

    def half_of(side):
        return pl.ds(side * (nz // 2), nz // 2)

    def hop_copy(v, side, to):
        sign = 1 - 2 * side
        return remote(
            part.at[v, plus_x(opposite), half_of(side)],
            hop_in.at[v, side],
            hs_sem.at[v, side],
            hr_sem.at[v, side],
            {"row_1": plus_x(sign * to)},
        )

    def half_copy(v, side, hopped, src, source, to):
        half_z = half_of(side if hopped else 1 - side)
        return remote(
            src if hopped else part.at[v, to, half_z],
            part_in.at[v, source, half_z],
            fs_sem.at[v, side, hopped],
            fr_sem.at[v, side, hopped],
            {"row_1": to},
        )

    def whole_copy(v, d, source, to):
        return remote(
            part.at[v, to], part_in.at[v, source], ps_sem.at[v, d % nx], pr_sem.at[v, source], {"row_1": to}
        )

    def start_sum(v):
        for side in range(2):
            hop_copy(v, side, 1).start()
        for d in sorted(whole, key=lambda d: -abs(d)):
            whole_copy(v, d, x, plus_x(d)).start()
        for side in range(2):
            half_copy(v, side, 0, None, x, plus_x((1 - 2 * side) * (opposite - 1))).start()

    def hop_on(v):
        for side in range(2):
            to = plus_x((1 - 2 * side) * (opposite - 1))
            hop_copy(v, side, 1).wait_recv()
            hop[v, side] = hop_in[v, side] + part[v, to, half_of(side)]
            half_copy(v, side, 1, hop.at[v, side], x, to).start()

    def sum_x(v):
        for d in whole:
            whole_copy(v, d, plus_x(d), plus_x(d)).wait_recv()
        for side in range(2):
            source = plus_x(-(1 - 2 * side) * (opposite - 1))
            for hopped in range(2):
                half_copy(v, side, hopped, hop.at[v, side], source, source).wait_recv()
        total = part[v, x]
        for d in range(1 - opposite, opposite):
            if d:
                total = total + part_in[v, plus_x(d)]
        mid[v] = total
        each_z(
            lambda d: remote(
                mid.at[v, plus_z(d)], mid_in.at[v, z], zs_sem.at[v, d], zr_sem.at[v, z], {"row_0": plus_z(d)}
            ).start()
        )

    def sum_z(v):
        each_z(
            lambda d: remote(
                mid.at[v, z], mid_in.at[v, z], zs_sem.at[v, d], zr_sem.at[v, plus_z(d)], {"row_0": z}
            ).wait_recv()
        )
        total = mid[v, z]
        for d in range(1, nz):
            total = total + mid_in[v, plus_z(d)]
        tile[v] = total

    def sent_sum(v):
        for d in whole:
            whole_copy(v, d, x, plus_x(d)).wait_send()
        for side in range(2):
            hop_copy(v, side, 1).wait_send()
            for hopped in range(2):
                half_copy(v, side, hopped, hop.at[v, side], x, plus_x(1)).wait_send()
        each_z(
            lambda d: remote(mid.at[v, z], mid.at[v, z], zs_sem.at[v, d], zr_sem.at[v, z], {"row_0": z}).wait_send()
        )

    def core_copy(src, dst, i):
        return remote(src, dst, cs_sem.at[i], cr_sem.at[i], {"col": other})

    loads = []
    for i, (src, dst) in enumerate(
        [
            (w_hbm, rows.at[0]),
            (c_hbm.at[pl.ds(half, half)], c_ref.at[0]),
            (p_hbm, rows.at[1]),
            (c_hbm.at[pl.ds(2 * half, half)], c_ref.at[1]),
            (x_hbm, rows.at[2]),
            (c_hbm.at[pl.ds(0, half)], c_ref.at[2]),
            (h_hbm, h_ref),
            (rv_hbm, rv_ref),
        ]
    ):
        loads.append(pltpu.make_async_copy(src, dst, in_sem.at[i]))
        loads[i].start()

    barrier = pltpu.get_barrier_semaphore()
    def signal(device):
        pl.semaphore_signal(barrier, inc=1, device_id=device, device_id_type=MESH)

    def both_cores(body):
        loop(1, 2 * nx, lambda n: body(n // nx, lax.rem(n, nx)))

    def core_of(which):
        return core + which * (1 - 2 * core)

    each_z(lambda d: signal({"row_0": plus_z(d)}))
    both_cores(lambda which, d: signal({"row_1": plus_x(d), "col": core_of(which)}))

    for load in loads[:6]:
        load.wait()

    rows[4] = jnp.zeros(rows.shape[1:], jnp.float32)

    def add_product(i):
        small_ref[2:4, :] = rows[4, 0:2, :]
        rows[4] += dot(rows[i], c_ref[i])

    loop(0, 3, add_product)
    small_ref[0:2, :] = rows[4, 0:2, :]
    for j in range(2):
        for q in range(2):
            nb_tile[j * 2 + q : j * 2 + q + 1, :] = rows[4, j : j + 1, q * LANES : (q + 1) * LANES]

    loads[6].wait()
    loads[7].wait()
    tiles = half // LANES

    def order(n):
        i = n // nx
        owner_x = lax.rem(n, nx)
        which = core + i - 2 * core * i
        for j in range(2):
            to = pl.multiple_of(j * owners + owner_x * nz, nz)
            for t in range(tiles):
                h_rows[i, pl.ds(to, nz), t * LANES : (t + 1) * LANES] = h_ref[
                    pl.ds(owner_x * 8 + (which * tiles + t) * 2 + j, nz, stride=8 * nx), :
                ]

    loop(0, 2 * nx, order)

    def own_product(v):
        prod[v] = dot(h_rows[0], rows[4 - 2 * v])

    loop(0, 2, own_product)
    pl.semaphore_wait(barrier, nz - 1 + 2 * nx - 1)
    y_core = core_copy(rows.at[4], rows.at[5], 1)
    y_core.start()
    x_core = core_copy(rows.at[2], rows.at[3], 0)
    x_core.start()
    send_all_z(nb_tile, nb_all_z, nzs_sem, nzr_sem)

    def other_product(v):
        @pl.when(v == 0)
        def _():
            y_core.wait_recv()

        @pl.when(v == 1)
        def _():
            x_core.wait_recv()

        value = prod[v] + dot(h_rows[1], rows[5 - 2 * v])
        for j in range(2):
            for q in range(2):
                block = value[j * owners : (j + 1) * owners, q * LANES : (q + 1) * LANES]
                part[v, :, :, j * 2 + q, :] = block.reshape(nx, nz, LANES)

        @pl.when(v == 1)
        def _():
            hop_on(0)

        start_sum(v)

    loop(0, 2, other_product)
    sum_x(0)
    hop_on(1)
    sum_x(1)

    got_all_z(nb_all_z, nzs_sem, nzr_sem)
    nb_all_z[z] = nb_tile[...]
    send_all_x(nb_all_z, gathered.at[0], nxs_sem, nxr_sem)
    gathered[0, x] = nb_all_z[...]

    sum_z(0)
    send_all_z(tile.at[0], all_z, gzs_sem, gzr_sem)
    all_z[z] = tile[0]

    sum_z(1)
    for q in range(2):
        squares = 0.0
        for j in range(2):
            columns = slice(q * LANES, (q + 1) * LANES)
            residual = tile[1, j * 2 + q : j * 2 + q + 1, :] - rows[2, j : j + 1, columns] * rv_ref[:, columns]
            small_ref[4 + j : 5 + j, columns] = residual
            squares = squares + residual * residual
        sq_tile[q : q + 1, :] = squares
    send_all_z(sq_tile, sq_all_z, qzs_sem, qzr_sem)
    sq_all_z[z] = sq_tile[...]

    def forward(n):
        k = groups - 1 - n
        group = far_group(k)
        members = pl.ds(group * GROUP, GROUP)

        def got_member(m):
            s = member(group, m)
            remote(all_z.at[s], all_z.at[s], gzs_sem.at[0], gzr_sem.at[s], {"row_0": z}).wait_recv()

        @pl.when(k < groups - 1)
        def _():
            got_member(0)

        loop(1, GROUP, got_member)
        loop(
            1,
            nx,
            lambda d: remote(
                all_z.at[members],
                gathered.at[1, x, members],
                gxs_sem.at[group, d],
                gxr_sem.at[group, x],
                {"row_1": plus_x(d)},
            ).start(),
        )

    loop(0, groups, forward)
    gathered[1, x] = all_z[...]

    def rows_of(u):
        columns = []
        for q in range(2):
            columns.append(
                jnp.concatenate([gathered[u, :, :, 2 * j + q, :].reshape(owners, LANES) for j in range(2)], axis=0)
            )
        return jnp.concatenate(columns, axis=1)

    got_all_x(gathered.at[0], nxs_sem, nxr_sem)
    nb_t[...] = rows_of(0).T

    def last_product(u):
        @pl.when(u == 1)
        def _():
            got_all_z(sq_all_z, qzs_sem, qzr_sem)
            sq_sum[...] = jnp.sum(sq_all_z[...], axis=0)
            both_cores(
                lambda which, d: remote(
                    sq_sum,
                    sq_all_x.at[core, x],
                    qxs_sem.at[which, d],
                    qxr_sem.at[core, x],
                    {"row_1": plus_x(d), "col": core_of(which)},
                ).start()
            )
            sq_all_x[core, x] = sq_sum[...]

            def got_group(group):
                members = pl.ds(group * GROUP, GROUP)
                each_x(
                    lambda d: remote(
                        all_z.at[members],
                        gathered.at[1, x, members],
                        gxs_sem.at[group, d],
                        gxr_sem.at[group, plus_x(d)],
                        {"row_1": x},
                    ).wait_recv()
                )

            loop(0, groups, got_group)

        core_own[u] = dot(nb_t[...], rows_of(u))
        remote(core_own.at[u], core_par.at[u], cs_sem.at[2 + u], cr_sem.at[2 + u], {"col": other}).start()

        @pl.when(u == 0)
        def _():
            y_core.wait_send()
            x_core.wait_send()
            sent_all_z(nb_tile, nzs_sem, nzr_sem)
            loop(0, 2, sent_sum)
            sent_all_x(nb_all_z, nxs_sem, nxr_sem)
            sent_all_z(tile.at[0], gzs_sem, gzr_sem)

        @pl.when(u == 1)
        def _():
            core_copy(core_own.at[0], core_par.at[0], 2).wait()
            metric_ref[...] = core_own[0] + core_par[0]
            sent_all_z(sq_tile, qzs_sem, qzr_sem)

            def sent_group(group):
                members = all_z.at[pl.ds(group * GROUP, GROUP)]
                each_x(
                    lambda d: remote(
                        members, members, gxs_sem.at[group, d], gxr_sem.at[group, x], {"row_1": x}
                    ).wait_send()
                )

            loop(0, groups, sent_group)

    small_ref[7:8, :] = jnp.zeros((1, small_ref.shape[1]), jnp.float32)
    loop(0, 2, last_product)
    core_copy(core_own.at[1], core_par.at[1], 3).wait()
    ritz_ref[...] = core_own[1] + core_par[1]
    both_cores(
        lambda which, d: remote(
            sq_sum,
            sq_all_x.at[core, x],
            qxs_sem.at[which, d],
            qxr_sem.at[core_of(which), plus_x(d)],
            {"row_1": x, "col": other},
        ).wait()
    )
    squares = jnp.sum(jnp.sum(sq_all_x[...], axis=0), axis=0)
    for q in range(2):
        small_ref[6:7, q * LANES : (q + 1) * LANES] = squares[q : q + 1, :]


def finish(window_total, small_in, ritz_in, metric_in, nb_ref, nd_ref, nc_ref, ritz_ref, metric_ref):
    ritz_ref[...] = ritz_in[...]
    metric_ref[...] = metric_in[...]
    nb_ref[...] = small_in[0:2, :]
    nd_ref[...] = small_in[2:4, :]
    nc_ref[...] = small_in[4:6, :] * lax.rsqrt(small_in[6:7, :] / window_total + 1e-06)


def on_device(hamiltonian_rows, current_block, correction_block, previous_block, ritz_values, mixing_coeffs):
    nz, nx = lax.axis_size("row_0"), lax.axis_size("row_1")
    groups = nz // GROUP
    owners, _, out_rows, columns = hamiltonian_rows.shape
    block_width = current_block.shape[1]
    window_total = out_rows * owners * lax.axis_size("col")
    tiles = columns // LANES
    h_flat = hamiltonian_rows.reshape(owners, out_rows, tiles, LANES).transpose(0, 2, 1, 3)
    h_flat = h_flat.reshape(owners * tiles * out_rows, LANES)
    f32 = functools.partial(jax.ShapeDtypeStruct, dtype=jnp.float32)
    vmem = pl.BlockSpec(memory_space=pltpu.VMEM)
    hbm = pl.BlockSpec(memory_space=pltpu.HBM)
    square = (block_width, block_width)

    def buffer(*shape):
        return pltpu.VMEM(shape, jnp.float32)

    sems = pltpu.SemaphoreType.DMA
    sem_shapes = (
        [(8,)]
        + [(2, nx)] * 2
        + [(2, 2, 2)] * 2
        + [(2, 2)] * 2
        + [(2, nz)] * 2
        + [(nz,)] * 2
        + [(groups, nx)] * 2
        + [(nz,)] * 2
        + [(2, nx)] * 2
        + [(nz,)] * 2
        + [(nx,)] * 2
        + [(4,)] * 2
    )
    chunk = (4, LANES)
    small, ritz, metric = pl.pallas_call(
        functools.partial(kernel, nz, nx),
        out_shape=(f32((8, block_width)), f32(square), f32(square)),
        in_specs=[hbm] * 6,
        out_specs=(vmem,) * 3,
        scratch_shapes=[
            buffer(1, block_width),
            buffer(*h_flat.shape),
            buffer(3, *square),
            buffer(6, *square),
            buffer(2, 2 * owners, block_width),
            buffer(2, 2 * owners, block_width),
            buffer(2, nx, nz, *chunk),
            buffer(2, nx, nz, *chunk),
            buffer(2, 2, nz // 2, *chunk),
            buffer(2, 2, nz // 2, *chunk),
            buffer(2, nz, *chunk),
            buffer(2, nz, *chunk),
            buffer(2, *chunk),
            buffer(nz, *chunk),
            buffer(2, nx, nz, *chunk),
            buffer(*chunk),
            buffer(nz, *chunk),
            buffer(block_width, 2 * owners),
            buffer(2, LANES),
            buffer(nz, 2, LANES),
            buffer(2, LANES),
            buffer(2, nx, 2, LANES),
            buffer(2, *square),
            buffer(2, *square),
        ]
        + [sems(shape) for shape in sem_shapes],
        compiler_params=pltpu.CompilerParams(
            collective_id=0, has_side_effects=True, vmem_limit_bytes=MAIN_VMEM
        ),
        name="lobpcg_step",
    )(
        *(
            pltpu.with_memory_space_constraint(a, pltpu.HBM)
            for a in (
                h_flat,
                current_block,
                correction_block,
                previous_block,
                mixing_coeffs,
                ritz_values.reshape(1, -1),
            )
        )
    )
    return pl.pallas_call(
        functools.partial(finish, window_total),
        out_shape=(f32((out_rows, block_width)),) * 3 + (f32(square),) * 2,
        in_specs=[vmem] * 3,
        out_specs=(vmem,) * 5,
        compiler_params=pltpu.CompilerParams(vmem_limit_bytes=END_VMEM),
        name="finish",
    )(small, ritz, metric)


def solution(mesh):
    finer = Mesh(
        mesh.devices.reshape(mesh.shape["chan"], NZ, NX, mesh.shape["col"]),
        ("chan", "row_0", "row_1", "col"),
    )
    in_specs = (
        P("chan", "col", None, ROW),
        P(CHAN_ROW_COL, None),
        P(CHAN_ROW_COL, None),
        P(CHAN_ROW_COL, None),
        P("chan"),
        P("chan", None),
    )
    out_specs = (
        P(CHAN_ROW_COL, None),
        P(CHAN_ROW_COL, None),
        P(CHAN_ROW_COL, None),
        P("chan", None),
        P("chan", None),
    )
    return jax.shard_map(on_device, mesh=finer, in_specs=in_specs, out_specs=out_specs, check_vma=False)
```

```python
import functools

import jax
import jax.numpy as jnp
from jax import lax
from jax.experimental import pallas as pl
from jax.experimental.pallas import tpu as pltpu
from jax.sharding import Mesh
from jax.sharding import PartitionSpec as P

NZ, NX = 16, 8
ROW = ("row_0", "row_1")
CHAN_ROW_COL = ("chan", "row_0", "row_1", "col")
MESH = pl.DeviceIdType.MESH
LANES = 128
GROUP = 4
MAIN_VMEM = 24 * 2**20
END_VMEM = 8 * 2**20
HIGHEST = lax.Precision.HIGHEST


def dot(left, right):
    return jnp.dot(left, right, preferred_element_type=jnp.float32, precision=HIGHEST)


def halves(value):
    high = value.astype(jnp.bfloat16)
    return high, (value - high.astype(jnp.float32)).astype(jnp.bfloat16)


def dot3(left, right):
    left_high, left_low = halves(left)
    right_high, right_low = halves(right)
    f32_dot = functools.partial(jnp.dot, preferred_element_type=jnp.float32)
    return f32_dot(left_high, right_high) + (f32_dot(left_high, right_low) + f32_dot(left_low, right_high))


def kernel(
    nz,
    nx,
    h_hbm,
    x_hbm,
    w_hbm,
    p_hbm,
    c_hbm,
    rv_hbm,
    small_ref,
    ritz_ref,
    metric_ref,
    rv_ref,
    h_ref,
    c_ref,
    rows,
    h_rows,
    prod,
    part,
    part_in,
    hop_in,
    hop,
    mid,
    mid_in,
    tile,
    all_z,
    gathered,
    nb_tile,
    nb_all_z,
    nb_t,
    sq_tile,
    sq_all_z,
    sq_sum,
    sq_all_x,
    core_own,
    core_par,
    in_sem,
    ps_sem,
    pr_sem,
    fs_sem,
    fr_sem,
    hs_sem,
    hr_sem,
    zs_sem,
    zr_sem,
    gzs_sem,
    gzr_sem,
    gxs_sem,
    gxr_sem,
    qzs_sem,
    qzr_sem,
    qxs_sem,
    qxr_sem,
    nzs_sem,
    nzr_sem,
    nxs_sem,
    nxr_sem,
    cs_sem,
    cr_sem,
):
    z = lax.axis_index("row_0")
    x = lax.axis_index("row_1")
    core = lax.axis_index("col")
    other = 1 - core
    owners = nz * nx
    groups = nz // GROUP
    own_group = z // GROUP
    half = rows.shape[1]

    def plus_z(d):
        return lax.rem(z + d, nz)

    def plus_x(d):
        return lax.rem(x + d + nx, nx)

    def far_group(k):
        step = (k + 1) // 2
        return lax.rem(own_group + groups // 2 + step * (1 - 2 * lax.rem(k, 2)) + groups, groups)

    def member(group, m):
        return group * GROUP + lax.rem(lax.rem(z, GROUP) + m, GROUP)

    def remote(src, dst, send, recv, device):
        return pltpu.make_async_remote_copy(
            src_ref=src, dst_ref=dst, send_sem=send, recv_sem=recv, device_id=device, device_id_type=MESH
        )

    def loop(first, last, body):
        def step(i, carry):
            body(i)
            return carry

        lax.fori_loop(first, last, step, 0)

    def far(i, n):
        return n // 2 + (i + 1) // 2 * (1 - 2 * lax.rem(i, 2))

    def each_z(body):
        loop(0, nz - 1, lambda i: body(far(i, nz)))

    def each_x(body):
        loop(0, nx - 1, lambda i: body(far(i, nx)))

    def send_all_z(src, into, s_sem, r_sem):
        each_z(lambda d: remote(src, into.at[z], s_sem.at[d], r_sem.at[z], {"row_0": plus_z(d)}).start())

    def got_all_z(into, s_sem, r_sem):
        each_z(lambda d: remote(into.at[z], into.at[z], s_sem.at[d], r_sem.at[plus_z(d)], {"row_0": z}).wait_recv())

    def sent_all_z(src, s_sem, r_sem):
        each_z(lambda d: remote(src, src, s_sem.at[d], r_sem.at[z], {"row_0": z}).wait_send())

    def send_all_x(src, into, s_sem, r_sem):
        each_x(lambda d: remote(src, into.at[x], s_sem.at[d], r_sem.at[x], {"row_1": plus_x(d)}).start())

    def got_all_x(into, s_sem, r_sem):
        each_x(lambda d: remote(into.at[x], into.at[x], s_sem.at[d], r_sem.at[plus_x(d)], {"row_1": x}).wait_recv())

    def sent_all_x(src, s_sem, r_sem):
        each_x(lambda d: remote(src, src, s_sem.at[d], r_sem.at[x], {"row_1": x}).wait_send())

    opposite = nx // 2
    whole = [d for d in range(1 - opposite, opposite) if abs(d) not in (0, opposite - 1)]

    def half_of(side):
        return pl.ds(side * (nz // 2), nz // 2)

    def hop_copy(v, side, to):
        sign = 1 - 2 * side
        return remote(
            part.at[v, plus_x(opposite), half_of(side)],
            hop_in.at[v, side],
            hs_sem.at[v, side],
            hr_sem.at[v, side],
            {"row_1": plus_x(sign * to)},
        )

    def half_copy(v, side, hopped, src, source, to):
        half_z = half_of(side if hopped else 1 - side)
        return remote(
            src if hopped else part.at[v, to, half_z],
            part_in.at[v, source, half_z],
            fs_sem.at[v, side, hopped],
            fr_sem.at[v, side, hopped],
            {"row_1": to},
        )

    def whole_copy(v, d, source, to):
        return remote(
            part.at[v, to], part_in.at[v, source], ps_sem.at[v, d % nx], pr_sem.at[v, source], {"row_1": to}
        )

    def start_sum(v):
        for side in range(2):
            hop_copy(v, side, 1).start()
        for d in sorted(whole, key=lambda d: -abs(d)):
            whole_copy(v, d, x, plus_x(d)).start()
        for side in range(2):
            half_copy(v, side, 0, None, x, plus_x((1 - 2 * side) * (opposite - 1))).start()

    def hop_on(v):
        for side in range(2):
            to = plus_x((1 - 2 * side) * (opposite - 1))
            hop_copy(v, side, 1).wait_recv()
            hop[v, side] = hop_in[v, side] + part[v, to, half_of(side)]
            half_copy(v, side, 1, hop.at[v, side], x, to).start()

    def sum_x(v):
        for d in whole:
            whole_copy(v, d, plus_x(d), plus_x(d)).wait_recv()
        for side in range(2):
            source = plus_x(-(1 - 2 * side) * (opposite - 1))
            for hopped in range(2):
                half_copy(v, side, hopped, hop.at[v, side], source, source).wait_recv()
        total = part[v, x]
        for d in range(1 - opposite, opposite):
            if d:
                total = total + part_in[v, plus_x(d)]
        mid[v] = total
        each_z(
            lambda d: remote(
                mid.at[v, plus_z(d)], mid_in.at[v, z], zs_sem.at[v, d], zr_sem.at[v, z], {"row_0": plus_z(d)}
            ).start()
        )

    def sum_z(v):
        each_z(
            lambda d: remote(
                mid.at[v, z], mid_in.at[v, z], zs_sem.at[v, d], zr_sem.at[v, plus_z(d)], {"row_0": z}
            ).wait_recv()
        )
        total = mid[v, z]
        for d in range(1, nz):
            total = total + mid_in[v, plus_z(d)]
        tile[v] = total

    def sent_sum(v):
        for d in whole:
            whole_copy(v, d, x, plus_x(d)).wait_send()
        for side in range(2):
            hop_copy(v, side, 1).wait_send()
            for hopped in range(2):
                half_copy(v, side, hopped, hop.at[v, side], x, plus_x(1)).wait_send()
        each_z(
            lambda d: remote(mid.at[v, z], mid.at[v, z], zs_sem.at[v, d], zr_sem.at[v, z], {"row_0": z}).wait_send()
        )

    def core_copy(src, dst, i):
        return remote(src, dst, cs_sem.at[i], cr_sem.at[i], {"col": other})

    barrier = pltpu.get_barrier_semaphore()
    def signal(device):
        pl.semaphore_signal(barrier, inc=1, device_id=device, device_id_type=MESH)

    def both_cores(body):
        loop(1, 2 * nx, lambda n: body(n // nx, lax.rem(n, nx)))

    def core_of(which):
        return core + which * (1 - 2 * core)

    each_z(lambda d: signal({"row_0": plus_z(d)}))
    both_cores(lambda which, d: signal({"row_1": plus_x(d), "col": core_of(which)}))

    loads = []
    for i, (src, dst) in enumerate(
        [
            (w_hbm, rows.at[0]),
            (c_hbm.at[pl.ds(half, half)], c_ref.at[0]),
            (p_hbm, rows.at[1]),
            (c_hbm.at[pl.ds(2 * half, half)], c_ref.at[1]),
            (x_hbm, rows.at[2]),
            (c_hbm.at[pl.ds(0, half)], c_ref.at[2]),
            (h_hbm, h_ref),
            (rv_hbm, rv_ref),
        ]
    ):
        loads.append(pltpu.make_async_copy(src, dst, in_sem.at[i]))
        loads[i].start()

    for load in loads[:6]:
        load.wait()

    rows[4] = jnp.zeros(rows.shape[1:], jnp.float32)

    def add_product(i):
        small_ref[2:4, :] = rows[4, 0:2, :]
        rows[4] += dot3(rows[i], c_ref[i])

    loop(0, 3, add_product)
    small_ref[0:2, :] = rows[4, 0:2, :]
    for j in range(2):
        for q in range(2):
            nb_tile[j * 2 + q : j * 2 + q + 1, :] = rows[4, j : j + 1, q * LANES : (q + 1) * LANES]

    loads[6].wait()
    loads[7].wait()
    tiles = half // LANES

    def order(n):
        i = n // nx
        owner_x = lax.rem(n, nx)
        which = core + i - 2 * core * i
        for j in range(2):
            to = pl.multiple_of(j * owners + owner_x * nz, nz)
            for t in range(tiles):
                h_rows[i, pl.ds(to, nz), t * LANES : (t + 1) * LANES] = h_ref[
                    pl.ds(owner_x * 8 + (which * tiles + t) * 2 + j, nz, stride=8 * nx), :
                ]

    loop(0, 2 * nx, order)

    prod[0] = dot3(h_rows[0], rows[4])
    prod[1] = dot(h_rows[0], rows[2])
    pl.semaphore_wait(barrier, nz - 1 + 2 * nx - 1)
    y_core = core_copy(rows.at[4], rows.at[5], 1)
    y_core.start()
    x_core = core_copy(rows.at[2], rows.at[3], 0)
    x_core.start()
    send_all_z(nb_tile, nb_all_z, nzs_sem, nzr_sem)

    def other_product(v):
        @pl.when(v == 0)
        def _():
            y_core.wait_recv()
            prod[0] += dot3(h_rows[1], rows[5])

        @pl.when(v == 1)
        def _():
            x_core.wait_recv()
            prod[1] += dot(h_rows[1], rows[3])

        for j in range(2):
            for q in range(2):
                block = prod[v, j * owners : (j + 1) * owners, q * LANES : (q + 1) * LANES]
                part[v, :, :, j * 2 + q, :] = block.reshape(nx, nz, LANES)

        @pl.when(v == 1)
        def _():
            hop_on(0)

        start_sum(v)

    loop(0, 2, other_product)
    sum_x(0)
    hop_on(1)
    sum_x(1)

    got_all_z(nb_all_z, nzs_sem, nzr_sem)
    nb_all_z[z] = nb_tile[...]
    send_all_x(nb_all_z, gathered.at[0], nxs_sem, nxr_sem)
    gathered[0, x] = nb_all_z[...]

    sum_z(0)
    send_all_z(tile.at[0], all_z, gzs_sem, gzr_sem)
    all_z[z] = tile[0]

    sum_z(1)
    for q in range(2):
        squares = 0.0
        for j in range(2):
            columns = slice(q * LANES, (q + 1) * LANES)
            residual = tile[1, j * 2 + q : j * 2 + q + 1, :] - rows[2, j : j + 1, columns] * rv_ref[:, columns]
            small_ref[4 + j : 5 + j, columns] = residual
            squares = squares + residual * residual
        sq_tile[q : q + 1, :] = squares
    send_all_z(sq_tile, sq_all_z, qzs_sem, qzr_sem)
    sq_all_z[z] = sq_tile[...]

    def forward(n):
        k = groups - 1 - n
        group = far_group(k)
        members = pl.ds(group * GROUP, GROUP)

        def got_member(m):
            s = member(group, m)
            remote(all_z.at[s], all_z.at[s], gzs_sem.at[0], gzr_sem.at[s], {"row_0": z}).wait_recv()

        @pl.when(k < groups - 1)
        def _():
            got_member(0)

        loop(1, GROUP, got_member)
        loop(
            1,
            nx,
            lambda d: remote(
                all_z.at[members],
                gathered.at[1, x, members],
                gxs_sem.at[group, d],
                gxr_sem.at[group, x],
                {"row_1": plus_x(d)},
            ).start(),
        )

    loop(0, groups, forward)
    gathered[1, x] = all_z[...]

    def rows_of(u):
        columns = []
        for q in range(2):
            columns.append(
                jnp.concatenate([gathered[u, :, :, 2 * j + q, :].reshape(owners, LANES) for j in range(2)], axis=0)
            )
        return jnp.concatenate(columns, axis=1)

    got_all_x(gathered.at[0], nxs_sem, nxr_sem)
    nb_t[...] = rows_of(0).T

    def last_product(u):
        @pl.when(u == 1)
        def _():
            got_all_z(sq_all_z, qzs_sem, qzr_sem)
            sq_sum[...] = jnp.sum(sq_all_z[...], axis=0)
            both_cores(
                lambda which, d: remote(
                    sq_sum,
                    sq_all_x.at[core, x],
                    qxs_sem.at[which, d],
                    qxr_sem.at[core, x],
                    {"row_1": plus_x(d), "col": core_of(which)},
                ).start()
            )
            sq_all_x[core, x] = sq_sum[...]

            def got_group(group):
                members = pl.ds(group * GROUP, GROUP)
                each_x(
                    lambda d: remote(
                        all_z.at[members],
                        gathered.at[1, x, members],
                        gxs_sem.at[group, d],
                        gxr_sem.at[group, plus_x(d)],
                        {"row_1": x},
                    ).wait_recv()
                )

            loop(0, groups, got_group)

        core_own[u] = dot3(nb_t[...], rows_of(u))
        remote(core_own.at[u], core_par.at[u], cs_sem.at[2 + u], cr_sem.at[2 + u], {"col": other}).start()

        @pl.when(u == 0)
        def _():
            y_core.wait_send()
            x_core.wait_send()
            sent_all_z(nb_tile, nzs_sem, nzr_sem)
            loop(0, 2, sent_sum)
            sent_all_x(nb_all_z, nxs_sem, nxr_sem)
            sent_all_z(tile.at[0], gzs_sem, gzr_sem)

        @pl.when(u == 1)
        def _():
            core_copy(core_own.at[0], core_par.at[0], 2).wait()
            metric_ref[...] = core_own[0] + core_par[0]
            sent_all_z(sq_tile, qzs_sem, qzr_sem)

            def sent_group(group):
                members = all_z.at[pl.ds(group * GROUP, GROUP)]
                each_x(
                    lambda d: remote(
                        members, members, gxs_sem.at[group, d], gxr_sem.at[group, x], {"row_1": x}
                    ).wait_send()
                )

            loop(0, groups, sent_group)

    small_ref[7:8, :] = jnp.zeros((1, small_ref.shape[1]), jnp.float32)
    loop(0, 2, last_product)
    core_copy(core_own.at[1], core_par.at[1], 3).wait()
    ritz_ref[...] = core_own[1] + core_par[1]
    both_cores(
        lambda which, d: remote(
            sq_sum,
            sq_all_x.at[core, x],
            qxs_sem.at[which, d],
            qxr_sem.at[core_of(which), plus_x(d)],
            {"row_1": x, "col": other},
        ).wait()
    )
    squares = jnp.sum(jnp.sum(sq_all_x[...], axis=0), axis=0)
    for q in range(2):
        small_ref[6:7, q * LANES : (q + 1) * LANES] = squares[q : q + 1, :]


def finish(window_total, small_in, ritz_in, metric_in, nb_ref, nd_ref, nc_ref, ritz_ref, metric_ref):
    ritz_ref[...] = ritz_in[...]
    metric_ref[...] = metric_in[...]
    nb_ref[...] = small_in[0:2, :]
    nd_ref[...] = small_in[2:4, :]
    nc_ref[...] = small_in[4:6, :] * lax.rsqrt(small_in[6:7, :] / window_total + 1e-06)


def on_device(hamiltonian_rows, current_block, correction_block, previous_block, ritz_values, mixing_coeffs):
    nz, nx = lax.axis_size("row_0"), lax.axis_size("row_1")
    groups = nz // GROUP
    owners, _, out_rows, columns = hamiltonian_rows.shape
    block_width = current_block.shape[1]
    window_total = out_rows * owners * lax.axis_size("col")
    tiles = columns // LANES
    h_flat = hamiltonian_rows.reshape(owners, out_rows, tiles, LANES).transpose(0, 2, 1, 3)
    h_flat = h_flat.reshape(owners * tiles * out_rows, LANES)
    f32 = functools.partial(jax.ShapeDtypeStruct, dtype=jnp.float32)
    vmem = pl.BlockSpec(memory_space=pltpu.VMEM)
    hbm = pl.BlockSpec(memory_space=pltpu.HBM)
    square = (block_width, block_width)

    def buffer(*shape):
        return pltpu.VMEM(shape, jnp.float32)

    sems = pltpu.SemaphoreType.DMA
    sem_shapes = (
        [(8,)]
        + [(2, nx)] * 2
        + [(2, 2, 2)] * 2
        + [(2, 2)] * 2
        + [(2, nz)] * 2
        + [(nz,)] * 2
        + [(groups, nx)] * 2
        + [(nz,)] * 2
        + [(2, nx)] * 2
        + [(nz,)] * 2
        + [(nx,)] * 2
        + [(4,)] * 2
    )
    chunk = (4, LANES)
    small, ritz, metric = pl.pallas_call(
        functools.partial(kernel, nz, nx),
        out_shape=(f32((8, block_width)), f32(square), f32(square)),
        in_specs=[hbm] * 6,
        out_specs=(vmem,) * 3,
        scratch_shapes=[
            buffer(1, block_width),
            buffer(*h_flat.shape),
            buffer(3, *square),
            buffer(6, *square),
            buffer(2, 2 * owners, block_width),
            buffer(2, 2 * owners, block_width),
            buffer(2, nx, nz, *chunk),
            buffer(2, nx, nz, *chunk),
            buffer(2, 2, nz // 2, *chunk),
            buffer(2, 2, nz // 2, *chunk),
            buffer(2, nz, *chunk),
            buffer(2, nz, *chunk),
            buffer(2, *chunk),
            buffer(nz, *chunk),
            buffer(2, nx, nz, *chunk),
            buffer(*chunk),
            buffer(nz, *chunk),
            buffer(block_width, 2 * owners),
            buffer(2, LANES),
            buffer(nz, 2, LANES),
            buffer(2, LANES),
            buffer(2, nx, 2, LANES),
            buffer(2, *square),
            buffer(2, *square),
        ]
        + [sems(shape) for shape in sem_shapes],
        compiler_params=pltpu.CompilerParams(
            collective_id=0, has_side_effects=True, vmem_limit_bytes=MAIN_VMEM
        ),
        name="lobpcg_step",
    )(
        *(
            pltpu.with_memory_space_constraint(a, pltpu.HBM)
            for a in (
                h_flat,
                current_block,
                correction_block,
                previous_block,
                mixing_coeffs,
                ritz_values.reshape(1, -1),
            )
        )
    )
    return pl.pallas_call(
        functools.partial(finish, window_total),
        out_shape=(f32((out_rows, block_width)),) * 3 + (f32(square),) * 2,
        in_specs=[vmem] * 3,
        out_specs=(vmem,) * 5,
        compiler_params=pltpu.CompilerParams(vmem_limit_bytes=END_VMEM),
        name="finish",
    )(small, ritz, metric)


def solution(mesh):
    finer = Mesh(
        mesh.devices.reshape(mesh.shape["chan"], NZ, NX, mesh.shape["col"]),
        ("chan", "row_0", "row_1", "col"),
    )
    in_specs = (
        P("chan", "col", None, ROW),
        P(CHAN_ROW_COL, None),
        P(CHAN_ROW_COL, None),
        P(CHAN_ROW_COL, None),
        P("chan"),
        P("chan", None),
    )
    out_specs = (
        P(CHAN_ROW_COL, None),
        P(CHAN_ROW_COL, None),
        P(CHAN_ROW_COL, None),
        P("chan", None),
        P("chan", None),
    )
    return jax.shard_map(on_device, mesh=finer, in_specs=in_specs, out_specs=out_specs, check_vma=False)
```
